256 devices in a mesh: row: 16 (over y, x), col: 16 (over z, core).
Axes of the slice: x: 4, y: 4, z: 8, core: 2. Of those that a mesh axis runs over, the one named last changes fastest.
Arguments:
- tokens: bfloat16 [256, 16384], P('row', 'col'), may hold values from -6 to 6
- grad_out: bfloat16 [256, 16384], P('row', 'col'), may hold values from -6 to 6
- w_gate: bfloat16 [16384, 26624], P('col', 'row'), may hold values from -0.046875 to 0.046875
- w_up: bfloat16 [16384, 26624], P('col', 'row'), may hold values from -0.046875 to 0.046875
- w_down: bfloat16 [26624, 16384], P('row', 'col'), may hold values from -0.0390625 to 0.0390625
- radius: float32 [1], replicated, may hold values from 8 to 24
Outputs:
- perturbed_out: bfloat16 [256, 16384], P('row', 'col')
- grad_norm: float32 [1], replicated
The draws below stay inside these ranges and needn't reach their ends.
All inputs are finite; a program needn't handle non-finite values.
Results may differ from the reference program's by a relative error of at most 0.02.
Values may be sent and summed in bfloat16 or wider, within the bound.
No kernel may reach another device: no remote copies, remote signals or barrier semaphores. Data moves between devices by JAX's collectives and lax.ppermute only.
A program may use at most 128 MiB of HBM per device.

```python
import math
import jax
import jax.numpy as jnp
from jax import lax

D = 16384
FFW = 26624
TOK = 256


def strengthened(drawn, own_key, source, target, blocks, factor):
    owner, partner = [(jnp.arange(drawn.shape[dim]) // (drawn.shape[dim] // blocks)).reshape([-1 if axis == dim else 1 for axis in range(drawn.ndim)]) for dim in (source, target)]
    chosen = jax.random.permutation(own_key, blocks)[partner]
    strong = (owner == chosen) | (owner == (partner + blocks // 2) % blocks)
    return jnp.where(strong, factor * drawn, drawn)


def block_scale(rng, extent, split, smallest, largest):
    level = 1.0
    for axis_at, parts in split:
        draws = jax.random.uniform(jax.random.fold_in(jax.random.fold_in(rng, 6), axis_at), (parts,), jnp.float32, smallest / len(split), largest / len(split))
        level = level * jnp.repeat(jnp.exp(draws), extent[axis_at] // parts).reshape((-1,) + (1,) * (len(extent) - 1 - axis_at))
    return level


def noise(rng, extent, deviation, bound, pieces=(), kind=jnp.bfloat16):
    drawn = jax.random.normal(rng, extent, jnp.float32) * deviation
    if len(pieces) > 0:
        drawn = block_scale(rng, extent, pieces, -0.22, 0.18) * drawn
    return jnp.clip(drawn, min=-bound, max=bound).astype(kind)


def heavy_noise(own_key, shape, scale, reach, split, heavy, kind=jnp.bfloat16):
    values = scale * jax.random.normal(own_key, shape, jnp.float32)
    if split:
        values = values * block_scale(own_key, shape, split, -0.22, 0.18)
    return jnp.clip(strengthened(values, jax.random.fold_in(own_key, 3), *heavy), -reach, reach).astype(kind)


def setup_inputs(seed: int = 0) -> dict:
    keys = jax.random.split(jax.random.key(seed), 7)
    tokens = heavy_noise(keys[0], (TOK, D), 1.0, 6.0, ((0, 16), (1, 16)), (1, 0, 16, 2.0))
    grad_out = heavy_noise(keys[1], (TOK, D), 1.0, 6.0, ((0, 16), (1, 16)), (1, 0, 16, 2.0))
    w_gate = noise(keys[2], (D, FFW), D ** -0.5, 0.046875, ((0, 16), (1, 16)))
    w_up = noise(keys[3], (D, FFW), D ** -0.5, 0.046875, ((0, 16), (1, 16)))
    w_down = noise(keys[4], (FFW, D), FFW ** -0.5, 0.0390625, ((0, 16), (1, 16)))
    radius = jnp.clip(jax.random.uniform(keys[5], (1,), jnp.float32, 8.0, 24.0), 8.0, 24.0)
    return {"tokens": tokens, "grad_out": grad_out, "w_gate": w_gate, "w_up": w_up, "w_down": w_down, "radius": radius}


def tdot(left, right):
    return lax.dot_general(left, right, (((0,), (0,)), ((), ())), preferred_element_type=jnp.float32)

def block_grads(tokens, grad_out, w_gate, w_up, w_down, index, width):
    start = (index * width).astype(jnp.int32)
    gate_blk = lax.dynamic_slice_in_dim(w_gate, start, width, 1)
    up_blk = lax.dynamic_slice_in_dim(w_up, start, width, 1)
    down_blk = lax.dynamic_slice_in_dim(w_down, start, width, 0)
    gate = jnp.dot(tokens, gate_blk, preferred_element_type=jnp.float32)
    upval = jnp.dot(tokens, up_blk, preferred_element_type=jnp.float32)
    sig = jax.nn.sigmoid(gate)
    silu = gate * sig
    hidden = (silu * upval).astype(jnp.bfloat16)
    grad_down = tdot(hidden, grad_out)
    grad_hidden = lax.dot_general(grad_out, down_blk, (((1,), (1,)), ((), ())), preferred_element_type=jnp.float32).astype(jnp.bfloat16).astype(jnp.float32)
    grad_gate_act = (grad_hidden * upval * sig * (1.0 + gate * (1.0 - sig))).astype(jnp.bfloat16)
    grad_up_act = (grad_hidden * silu).astype(jnp.bfloat16)
    grad_gate = tdot(tokens, grad_gate_act)
    grad_up = tdot(tokens, grad_up_act)
    return (grad_gate, grad_up, grad_down, gate_blk, up_blk, down_blk)

def reference(tokens, grad_out, w_gate, w_up, w_down, radius):
    nblocks = math.gcd(FFW, 16)
    width = FFW // nblocks
    indices = jnp.arange(nblocks, dtype=jnp.int32)

    def first(carry, index):
        grad_gate, grad_up, grad_down, a_blk, b_blk, c_blk = block_grads(tokens, grad_out, w_gate, w_up, w_down, index, width)
        part = jnp.sum(grad_gate * grad_gate) + jnp.sum(grad_up * grad_up) + jnp.sum(grad_down * grad_down)
        return (carry + part, None)
    total, unused = lax.scan(first, jnp.zeros((), jnp.float32), indices)
    scale = radius[0] * lax.rsqrt(total + 1e-06)

    def second(carry, index):
        grad_gate, grad_up, grad_down, gate_blk, up_blk, down_blk = block_grads(tokens, grad_out, w_gate, w_up, w_down, index, width)
        gate_pert = (gate_blk.astype(jnp.float32) + scale * grad_gate).astype(jnp.bfloat16)
        up_pert = (up_blk.astype(jnp.float32) + scale * grad_up).astype(jnp.bfloat16)
        down_pert = (down_blk.astype(jnp.float32) + scale * grad_down).astype(jnp.bfloat16)
        pgate = jnp.dot(tokens, gate_pert, preferred_element_type=jnp.float32)
        pup = jnp.dot(tokens, up_pert, preferred_element_type=jnp.float32)
        phidden = (jax.nn.silu(pgate) * pup).astype(jnp.bfloat16)
        return (carry + jnp.dot(phidden, down_pert, preferred_element_type=jnp.float32), None)
    summed, unused = lax.scan(second, jnp.zeros((TOK, D), jnp.float32), indices)
    return (summed.astype(jnp.bfloat16), jnp.sqrt(total).reshape(1))
```

```python
import jax
import jax.numpy as jnp
from jax import lax
from jax.sharding import Mesh
from jax.sharding import PartitionSpec as P

ROW = ("row_0", "row_1")
COL = ("col_0", "col_1")
Z = "col_0"
CORE = "col_1"
F32 = jnp.float32
BF16 = jnp.bfloat16


def dot(left, right, over):
    return lax.dot_general(
        left, right, (((over[0],), (over[1],)), ((), ())), preferred_element_type=F32
    )


def to_all(x, axis):
    copies = jnp.broadcast_to(x[None], (lax.axis_size(axis), *x.shape))
    return lax.all_to_all(copies, axis, 0, 0, tiled=True)


def swap_cores(x):
    return lax.ppermute(x, CORE, [(0, 1), (1, 0)])


def sum_everywhere(x, axis):
    tile = jnp.broadcast_to(x, (8, 128))
    return jnp.sum(to_all(tile, axis)[:, 0, 0])


def per_device(tokens, grad_out, w_gate, w_up, w_down, radius):
    core = lax.axis_index(CORE)
    peers = lax.axis_size(Z)
    rows = tokens.shape[0]
    ours = to_all(jnp.concatenate([tokens, grad_out], 0), ROW)
    x = ours[:, :rows].reshape(-1, tokens.shape[1])
    dy = ours[:, rows:].reshape(-1, tokens.shape[1])
    half = x.shape[0] // 2

    def theirs_then_mine(a):
        return jnp.concatenate(
            [
                lax.dynamic_slice_in_dim(a, (1 - core) * half, half, 0),
                lax.dynamic_slice_in_dim(a, core * half, half, 0),
            ],
            0,
        )

    x_ord, dy_ord = theirs_then_mine(x), theirs_then_mine(dy)
    terms = [
        dot(w_gate, x_ord, (0, 1)),
        dot(w_up, x_ord, (0, 1)),
        dot(w_down, dy_ord, (1, 1)),
        dot(x, x_ord, (1, 1)),
        dot(dy, dy_ord, (1, 1)),
    ]
    terms = jnp.concatenate([t.astype(BF16).reshape(peers, -1, 2 * half) for t in terms], 1)
    arrived = swap_cores(terms[:, :, :half])
    chip = (terms[:, :, half:].astype(F32) + arrived.astype(F32)).astype(BF16)
    summed = jnp.sum(lax.all_to_all(chip, Z, 0, 0, tiled=True).astype(F32), 0)
    width = w_gate.shape[1] // peers
    slab = 2 * half // peers
    gate = summed[:width]
    up = summed[width : 2 * width]
    grad_hidden = summed[2 * width : 3 * width].astype(BF16).astype(F32)
    grams = to_all(summed[3 * width :].astype(BF16), Z)
    gram_x = theirs_then_mine(grams[:, :slab].reshape(2 * half, half))
    gram_y = theirs_then_mine(grams[:, slab:].reshape(2 * half, half))

    sig = jax.nn.sigmoid(gate)
    silu = gate * sig
    hidden = (silu * up).astype(BF16)
    grad_gate_act = (grad_hidden * up * sig * (1.0 + gate * (1.0 - sig))).astype(BF16)
    grad_up_act = (grad_hidden * silu).astype(BF16)
    acts = jnp.concatenate([hidden, grad_gate_act, grad_up_act], 0)
    acts = jnp.concatenate([swap_cores(acts), acts], 1)
    down_step = dot(acts[:width], gram_y, (1, 0))
    step = dot(acts[width:], gram_x, (1, 0))
    local = jnp.sum(hidden.astype(F32) * down_step) + jnp.sum(
        acts[width:, half:].astype(F32) * step
    )
    total = sum_everywhere(sum_everywhere(local, ROW), COL)
    scale = radius[0] * lax.rsqrt(total + 1e-06)
    pgate = gate + scale * step[:width]
    pup = up + scale * step[width:]
    phidden = (jax.nn.silu(pgate) * pup).astype(BF16)

    mine = to_all(jnp.concatenate([phidden, hidden], 0), Z)
    theirs = swap_cores(mine)
    both = jnp.concatenate([theirs, mine], 2)
    ph = both[:, :width].reshape(-1, 2 * half)
    h = both[:, width:].reshape(-1, 2 * half)
    mix = (scale * dot(ph, h, (0, 0))).astype(BF16)
    partial_out = dot(ph, w_down, (0, 0)) + dot(mix, dy_ord, (1, 0))
    partial_out = theirs_then_mine(partial_out.astype(BF16))
    blocks = partial_out.reshape(-1, rows, partial_out.shape[1])
    parts = lax.all_to_all(blocks, ROW, 0, 0, tiled=True)
    return (jnp.sum(parts.astype(F32), 0).astype(BF16), jnp.sqrt(total).reshape(1))


def solution(mesh):
    split = Mesh(mesh.devices.reshape(4, 4, 8, 2), ("row_0", "row_1", "col_0", "col_1"))
    return jax.shard_map(
        per_device,
        mesh=split,
        in_specs=(P(ROW, COL), P(ROW, COL), P(COL, ROW), P(COL, ROW), P(ROW, COL), P()),
        out_specs=(P(ROW, COL), P()),
        check_vma=False,
    )
```

```python
import jax
import jax.numpy as jnp
from jax import lax
from jax.experimental import pallas as pl
from jax.experimental.pallas import tpu as pltpu
from jax.sharding import Mesh
from jax.sharding import PartitionSpec as P

ROW = ("row_0", "row_1")
COL = ("col_0", "col_1")
Z = "col_0"
CORE = "col_1"
F32 = jnp.float32
BF16 = jnp.bfloat16
LANES = 128


def dot(left, right, over):
    return lax.dot_general(
        left, right, (((over[0],), (over[1],)), ((), ())), preferred_element_type=F32
    )


def to_all(x, axis):
    copies = jnp.broadcast_to(x[None], (lax.axis_size(axis), *x.shape))
    return lax.all_to_all(copies, axis, 0, 0, tiled=True)


def swap_cores(x):
    return lax.ppermute(x, CORE, [(0, 1), (1, 0)])


def sum_everywhere(x, axis):
    tile = jnp.broadcast_to(x, (8, LANES))
    return jnp.sum(to_all(tile, axis)[:, 0, 0])


def put_halves(core, block, at, theirs_ref, mine_ref):
    half = block.shape[2] // 2
    n = block.shape[1]
    low, high = block[:, :, :half], block[:, :, half:]
    theirs_ref[:, pl.ds(at, n), :] = jnp.where(core == 0, high, low).astype(BF16)
    mine_ref[:, pl.ds(at, n), :] = jnp.where(core == 0, low, high).astype(BF16)


def gate_up_kernel(core_ref, x_ref, wg_ref, wu_ref, theirs_ref, mine_ref):
    j = pl.program_id(0)
    core = core_ref[0]
    x = x_ref[...]
    peers = theirs_ref.shape[0]
    tokens = x.shape[0]
    slab = tokens // peers
    part = LANES // peers
    width = (theirs_ref.shape[1] - slab) // 2
    w = jnp.concatenate([wg_ref[...], wu_ref[...]], 1)
    both = jnp.dot(x, w, preferred_element_type=F32).T
    at = pl.multiple_of(j * part, part)
    put_halves(core, both[:LANES].reshape(peers, part, tokens), at, theirs_ref, mine_ref)
    put_halves(core, both[LANES:].reshape(peers, part, tokens), width + at, theirs_ref, mine_ref)

    @pl.when(j == 0)
    def _():
        gram = dot(x, x, (1, 1))
        put_halves(core, gram.reshape(peers, slab, tokens), 2 * width, theirs_ref, mine_ref)


def gate_up_terms(core, x, w_gate, w_up, peers):
    depth, hidden = w_gate.shape
    tokens = x.shape[0]
    rows = 2 * hidden // peers + tokens // peers
    out = jax.ShapeDtypeStruct((peers, rows, tokens // 2), BF16)
    whole = pl.BlockSpec(out.shape, lambda j: (0, 0, 0))
    return pl.pallas_call(
        gate_up_kernel,
        grid=(hidden // LANES,),
        in_specs=[
            pl.BlockSpec(memory_space=pltpu.SMEM),
            pl.BlockSpec((tokens, depth), lambda j: (0, 0)),
            pl.BlockSpec((depth, LANES), lambda j: (0, j)),
            pl.BlockSpec((depth, LANES), lambda j: (0, j)),
        ],
        out_specs=[whole, whole],
        out_shape=[out, out],
        cost_estimate=pl.CostEstimate(
            flops=4 * tokens * depth * hidden, bytes_accessed=4 * depth * hidden, transcendentals=0
        ),
        name="gate_up_terms",
    )(core, x, w_gate, w_up)


def hidden_grad_kernel(core_ref, dy_ref, wd_ref, theirs_ref, mine_ref):
    j = pl.program_id(0)
    peers = theirs_ref.shape[0]
    part = LANES // peers
    block = dot(wd_ref[...], dy_ref[...], (1, 1))
    at = pl.multiple_of(j * part, part)
    put_halves(core_ref[0], block.reshape(peers, part, block.shape[1]), at, theirs_ref, mine_ref)


def hidden_grad_terms(core, dy, w_down, peers):
    hidden, depth = w_down.shape
    tokens = dy.shape[0]
    out = jax.ShapeDtypeStruct((peers, hidden // peers, tokens // 2), BF16)
    whole = pl.BlockSpec(out.shape, lambda j: (0, 0, 0))
    return pl.pallas_call(
        hidden_grad_kernel,
        grid=(hidden // LANES,),
        in_specs=[
            pl.BlockSpec(memory_space=pltpu.SMEM),
            pl.BlockSpec((tokens, depth), lambda j: (0, 0)),
            pl.BlockSpec((LANES, depth), lambda j: (j, 0)),
        ],
        out_specs=[whole, whole],
        out_shape=[out, out],
        cost_estimate=pl.CostEstimate(
            flops=2 * tokens * depth * hidden, bytes_accessed=2 * depth * hidden, transcendentals=0
        ),
        name="hidden_grad_terms",
    )(core, dy, w_down)


def out_kernel(core_ref, scale_ref, pt_ref, pm_ref, ht_ref, hm_ref, wd_ref, dy_ref, out_ref, ph_ref, mix_ref):
    peers, width, half = pm_ref.shape
    part = LANES // peers

    @pl.when(pl.program_id(0) == 0)
    def _():
        for at, p_ref in ((0, pt_ref), (half, pm_ref)):
            for j in range(width // part):
                block = p_ref[:, j * part : (j + 1) * part, :].reshape(LANES, half)
                ph_ref[at : at + half, j * LANES : (j + 1) * LANES] = block.astype(F32).T.astype(BF16)
        for a, p_ref in ((0, pt_ref), (half, pm_ref)):
            for b, h_ref in ((0, ht_ref), (half, hm_ref)):
                p = p_ref[...].reshape(peers * width, half)
                h = h_ref[...].reshape(peers * width, half)
                mix_ref[a : a + half, b : b + half] = (scale_ref[0] * dot(p, h, (0, 0))).astype(BF16)

    acc = dot(ph_ref[...], wd_ref[...], (1, 0)) + dot(mix_ref[...], dy_ref[...], (1, 0))
    out = acc.astype(BF16)
    theirs = pl.multiple_of((1 - core_ref[0]) * half, half)
    mine = pl.multiple_of(core_ref[0] * half, half)
    out_ref[pl.ds(theirs, half), :] = out[:half]
    out_ref[pl.ds(mine, half), :] = out[half:]


def out_terms(core, scale, ph_theirs, ph_mine, h_theirs, h_mine, w_down, dy):
    hidden, depth = w_down.shape
    tokens = dy.shape[0]
    block = min(depth, 256)
    slab = pl.BlockSpec(ph_mine.shape, lambda n: (0, 0, 0))
    return pl.pallas_call(
        out_kernel,
        grid=(depth // block,),
        in_specs=[
            pl.BlockSpec(memory_space=pltpu.SMEM),
            pl.BlockSpec(memory_space=pltpu.SMEM),
            slab,
            slab,
            slab,
            slab,
            pl.BlockSpec((hidden, block), lambda n: (0, n)),
            pl.BlockSpec((tokens, block), lambda n: (0, n)),
        ],
        out_specs=pl.BlockSpec((tokens, block), lambda n: (0, n)),
        out_shape=jax.ShapeDtypeStruct((tokens, depth), BF16),
        scratch_shapes=[pltpu.VMEM((tokens, hidden), BF16), pltpu.VMEM((tokens, tokens), BF16)],
        cost_estimate=pl.CostEstimate(
            flops=2 * tokens * depth * hidden, bytes_accessed=2 * depth * hidden, transcendentals=0
        ),
        name="out_terms",
    )(core, scale, ph_theirs, ph_mine, h_theirs, h_mine, w_down, dy)


def add_halves(mine, arrived):
    return (mine.astype(F32) + arrived.astype(F32)).astype(BF16)


def sum_at_owner(x):
    return jnp.sum(lax.all_to_all(x, Z, 0, 0, tiled=True).astype(F32), 0)


def per_device(tokens, grad_out, w_gate, w_up, w_down, radius):
    core = lax.axis_index(CORE)
    which = core.reshape(1).astype(jnp.int32)
    peers = lax.axis_size(Z)
    rows, depth = tokens.shape

    def theirs_then_mine(a, half):
        return jnp.concatenate(
            [
                lax.dynamic_slice_in_dim(a, (1 - core) * half, half, 0),
                lax.dynamic_slice_in_dim(a, core * half, half, 0),
            ],
            0,
        )

    x = to_all(tokens, ROW).reshape(-1, depth)
    half = x.shape[0] // 2
    theirs, mine = gate_up_terms(which, x, w_gate, w_up, peers)
    arrived = swap_cores(theirs)
    chip = add_halves(mine, arrived)
    summed = sum_at_owner(chip)
    own_dy = lax.optimization_barrier((grad_out, chip))[0]
    dy = lax.all_gather(own_dy, ROW, axis=0, tiled=True)
    dy_ord = theirs_then_mine(dy, half)
    theirs, mine = hidden_grad_terms(which, dy, w_down, peers)
    arrived = swap_cores(theirs)
    chip_gh = add_halves(mine, arrived)
    width = w_gate.shape[1] // peers
    gate = summed[:width]
    up = summed[width : 2 * width]

    sig = jax.nn.sigmoid(gate)
    silu = gate * sig
    hidden = (silu * up).astype(BF16)
    shared = jnp.concatenate([hidden, summed[2 * width :].astype(BF16)], 0)
    shared = jnp.broadcast_to(shared[None], (peers, *shared.shape))
    fetched = lax.all_to_all(jnp.concatenate([chip_gh, shared], 1), Z, 0, 0, tiled=True)
    grad_hidden = jnp.sum(fetched[:, :width].astype(F32), 0).astype(BF16).astype(F32)
    h_mine = fetched[:, width : 2 * width]
    gram_x = theirs_then_mine(fetched[:, 2 * width :].reshape(2 * half, half), half)
    h_theirs = swap_cores(h_mine)
    gram_y = dot(dy_ord, dy_ord, (1, 1)).astype(BF16)
    h_all = jnp.concatenate([h_theirs, h_mine], 2).reshape(-1, 2 * half)
    down_square = jnp.sum(dot(h_all, gram_y, (1, 0)) * h_all.astype(F32))

    grad_gate_act = (grad_hidden * up * sig * (1.0 + gate * (1.0 - sig))).astype(BF16)
    grad_up_act = (grad_hidden * silu).astype(BF16)
    acts = jnp.concatenate([grad_gate_act, grad_up_act], 0)
    acts_theirs = swap_cores(acts)
    step = dot(jnp.concatenate([acts_theirs, acts], 1), gram_x, (1, 0))
    local = jnp.sum(acts.astype(F32) * step) + down_square
    total = sum_everywhere(local, (*ROW, CORE))
    total = sum_everywhere(total, Z)
    scale = radius[0] * lax.rsqrt(total + 1e-06)
    pgate = gate + scale * step[:width]
    pup = up + scale * step[width:]
    phidden = (jax.nn.silu(pgate) * pup).astype(BF16)

    ph_mine = to_all(phidden, Z)
    ph_theirs = swap_cores(ph_mine)
    partial_out = out_terms(
        which, scale.reshape(1), ph_theirs, ph_mine, h_theirs, h_mine, w_down, dy_ord
    )
    blocks = partial_out.reshape(-1, rows, depth)
    parts = lax.all_to_all(blocks, ROW, 0, 0, tiled=True)
    return (jnp.sum(parts.astype(F32), 0).astype(BF16), jnp.sqrt(total).reshape(1))


def solution(mesh):
    split = Mesh(mesh.devices.reshape(4, 4, 8, 2), ("row_0", "row_1", "col_0", "col_1"))
    return jax.shard_map(
        per_device,
        mesh=split,
        in_specs=(P(ROW, COL), P(ROW, COL), P(COL, ROW), P(COL, ROW), P(ROW, COL), P()),
        out_specs=(P(ROW, COL), P()),
        check_vma=False,
    )
```

```python
import jax
import jax.numpy as jnp
from jax import lax
from jax.experimental import pallas as pl
from jax.experimental.pallas import tpu as pltpu
from jax.sharding import Mesh
from jax.sharding import PartitionSpec as P

ROW = ("row_0", "row_1")
COL = ("col_0", "col_1")
Z = "col_0"
CORE = "col_1"
F32 = jnp.float32
BF16 = jnp.bfloat16
LANES = 128
SUBLANES = 8
MIB = 1 << 20
VMEM = pl.BlockSpec(memory_space=pltpu.VMEM)
SMEM = pl.BlockSpec(memory_space=pltpu.SMEM)


def dot(left, right, over):
    return lax.dot_general(
        left, right, (((over[0],), (over[1],)), ((), ())), preferred_element_type=F32
    )


def exchange(x, axis):
    return lax.all_to_all(x, axis, 0, 0, tiled=True)


def swap_cores(x):
    return lax.ppermute(x, CORE, [(0, 1), (1, 0)])


def local_kernel(body, out_shape, operands, limit=16, flops=1_000_000):
    return pl.pallas_call(
        body,
        in_specs=[SMEM if a.dtype == jnp.int32 else VMEM for a in operands],
        out_specs=[VMEM] * len(out_shape),
        out_shape=[jax.ShapeDtypeStruct(*shape) for shape in out_shape],
        compiler_params=pltpu.CompilerParams(vmem_limit_bytes=limit * MIB),
        cost_estimate=pl.CostEstimate(flops=flops, bytes_accessed=1_000_000, transcendentals=0),
    )(*operands)


def copies_in_kernel(tokens_ref, dy_ref, out_ref, done):
    rows = tokens_ref.shape[0]
    copies = [
        pltpu.make_async_copy(
            own_ref, out_ref.at[peer, kind * rows : (kind + 1) * rows], done.at[peer, kind]
        )
        for peer in range(out_ref.shape[0])
        for kind, own_ref in enumerate((tokens_ref, dy_ref))
    ]
    for copy in copies:
        copy.start()
    for copy in copies:
        copy.wait()


def copies_in(tokens, grad_out, sources):
    rows, depth = tokens.shape
    return pl.pallas_call(
        copies_in_kernel,
        in_specs=[pl.BlockSpec(memory_space=pl.ANY)] * 2,
        out_specs=VMEM,
        out_shape=jax.ShapeDtypeStruct((sources, 2 * rows, depth), BF16),
        scratch_shapes=[pltpu.SemaphoreType.DMA((sources, 2))],
        cost_estimate=pl.CostEstimate(flops=1_000_000, bytes_accessed=1_000_000, transcendentals=0),
        name="copies_in",
    )(tokens, grad_out)


def terms_kernel(
    core_ref, in_ref, wg_ref, wu_ref, wd_ref, theirs_ref, mine_ref, ord_ref, prod_ref, w_ref, down_ref, arrived
):
    j = pl.program_id(0)
    steps = w_ref.shape[0]
    peers = theirs_ref.shape[0]
    sources, rows2, depth = in_ref.shape
    rows = rows2 // 2
    tokens = sources * rows
    half = tokens // 2
    slab = tokens // peers
    part = LANES // peers
    width = steps * part
    core = core_ref[0]
    sides = ((1 - core, theirs_ref), (core, mine_ref))

    def fetch(step, kind):
        at = pl.multiple_of(step * LANES, LANES)
        if kind == 2:
            source, target = wd_ref.at[pl.ds(at, LANES)], down_ref.at[pl.ds(at, LANES)]
        else:
            source = (wg_ref, wu_ref)[kind].at[:, pl.ds(at, LANES)]
            target = w_ref.at[step, :, pl.ds(kind * LANES, LANES)]
        return pltpu.make_async_copy(source, target, arrived.at[step, kind])

    @pl.when(j == 0)
    def _():
        for step in range(steps):
            fetch(step, 0).start()
            fetch(step, 1).start()
        for step in range(steps):
            fetch(step, 2).start()
        for kind in range(2):
            row_at = 2 * width + kind * slab
            a = in_ref[:, kind * rows : (kind + 1) * rows, :].reshape(tokens, depth)
            for side, out_ref in sides:
                own = in_ref[
                    pl.ds(side * (sources // 2), sources // 2), kind * rows : (kind + 1) * rows, :
                ].reshape(half, depth)
                gram = dot(a, own, (1, 1)).astype(BF16)
                out_ref[:, row_at : row_at + slab, :] = gram.reshape(peers, slab, half)
        for at, side in ((0, 1 - core), (half, core)):
            own = in_ref[pl.ds(side * (sources // 2), sources // 2), rows:, :]
            ord_ref[at : at + half] = own.reshape(half, depth)

    last = pl.multiple_of(jnp.maximum(j - 1, 0) * part, part)
    for side, out_ref in sides:
        token_at = pl.multiple_of(side * half, half)
        block = prod_ref[lax.rem(j + 1, 2), pl.ds(token_at, half), :].T.astype(BF16)
        out_ref[:, pl.ds(last, part), :] = block[:LANES].reshape(peers, part, half)
        out_ref[:, pl.ds(width + last, part), :] = block[LANES:].reshape(peers, part, half)
    x = in_ref[:, :rows, :].reshape(tokens, depth)
    now = jnp.minimum(j, steps - 1)

    @pl.when(j < steps)
    def _():
        fetch(now, 0).wait()
        fetch(now, 1).wait()

    prod_ref[lax.rem(j, 2)] = jnp.dot(x, w_ref[now], preferred_element_type=F32)

    @pl.when(j == steps)
    def _():
        for step in range(steps):
            fetch(step, 2).wait()
        for first in range(0, steps, 4):
            end = min(first + 4, steps)
            rows_in = slice(first * LANES, end * LANES)
            block = dot(down_ref[rows_in], ord_ref[...], (1, 1)).astype(BF16)
            for step in range(first, end):
                piece = block[(step - first) * LANES : (step - first + 1) * LANES]
                piece = piece.reshape(peers, part, tokens)
                to = 2 * width + 2 * slab + step * part
                theirs_ref[:, to : to + part, :] = piece[:, :, :half]
                mine_ref[:, to : to + part, :] = piece[:, :, half:]


def terms(core, fetched, w_gate, w_up, w_down, peers):
    depth, hidden = w_gate.shape
    tokens = fetched.shape[0] * fetched.shape[1] // 2
    steps = hidden // LANES
    rows = 3 * hidden // peers + 2 * tokens // peers
    out = jax.ShapeDtypeStruct((peers, rows, tokens // 2), BF16)
    dy = jax.ShapeDtypeStruct((tokens, depth), BF16)
    whole = pl.BlockSpec(out.shape, lambda j: (0, 0, 0))
    hbm = pl.BlockSpec(memory_space=pl.ANY)
    return pl.pallas_call(
        terms_kernel,
        grid=(steps + 1,),
        in_specs=[SMEM, pl.BlockSpec(fetched.shape, lambda j: (0, 0, 0)), hbm, hbm, hbm],
        out_specs=[whole, whole, pl.BlockSpec(dy.shape, lambda j: (0, 0))],
        out_shape=[out, out, dy],
        scratch_shapes=[
            pltpu.VMEM((2, tokens, 2 * LANES), F32),
            pltpu.VMEM((steps, depth, 2 * LANES), BF16),
            pltpu.VMEM((hidden, depth), BF16),
            pltpu.SemaphoreType.DMA((steps, 3)),
        ],
        compiler_params=pltpu.CompilerParams(vmem_limit_bytes=TERMS_MIB * MIB),
        cost_estimate=pl.CostEstimate(
            flops=6 * tokens * depth * hidden, bytes_accessed=6 * depth * hidden, transcendentals=0
        ),
        name="terms",
    )(core, fetched, w_gate, w_up, w_down)


def add_kernel(a_ref, b_ref, first_ref, second_ref):
    rows = first_ref.shape[1]
    both = (a_ref[...].astype(F32) + b_ref[...].astype(F32)).astype(BF16)
    first_ref[...] = both[:, :rows]
    second_ref[...] = both[:, rows:]


def middle_kernel(sums_ref, grad_ref, sent_ref, gate_ref, up_ref):
    peers, _, _ = sums_ref.shape
    width = grad_ref.shape[1]
    total = sums_ref[0].astype(F32)
    for peer in range(1, peers):
        total = total + sums_ref[peer].astype(F32)
    gate_ref[...] = total[:width]
    up_ref[...] = total[width : 2 * width]
    grams = total[2 * width :].astype(BF16)
    sent_ref[:, :width, :] = grad_ref[...]
    for peer in range(peers):
        sent_ref[peer, width:, :] = grams


def acts_kernel(sums_ref, gate_ref, up_ref, acts_ref):
    width = gate_ref.shape[0]
    total = sums_ref[0, :width].astype(F32)
    for peer in range(1, sums_ref.shape[0]):
        total = total + sums_ref[peer, :width].astype(F32)
    grad_hidden = total.astype(BF16).astype(F32)
    gate, up = gate_ref[...], up_ref[...]
    sig = jax.nn.sigmoid(gate)
    silu = gate * sig
    acts_ref[:width] = (grad_hidden * up * sig * (1.0 + gate * (1.0 - sig))).astype(BF16)
    acts_ref[width : 2 * width] = (grad_hidden * silu).astype(BF16)
    acts_ref[2 * width :] = (silu * up).astype(BF16)


def step_kernel(core_ref, acts_ref, arrived_ref, grams_ref, step_ref, local_ref):
    peers, rows, half = grams_ref.shape
    width = acts_ref.shape[0] // 3
    slab = (rows - width) // 2
    core = core_ref[0]
    kinds = ((0, 2 * width, width), (2 * width, 3 * width, width + slab))
    local = 0.0
    for first, end, at in kinds:
        product = 0.0
        for side, part_ref in ((1 - core, arrived_ref), (core, acts_ref)):
            gram = grams_ref[pl.ds(side * (peers // 2), peers // 2), at : at + slab, :]
            product += dot(part_ref[first:end], gram.reshape(half, half), (1, 0))
        local += jnp.sum(acts_ref[first:end].astype(F32) * product)
        if first == 0:
            step_ref[...] = product
    local_ref[...] = jnp.full(local_ref.shape, local, F32)


def norm_kernel(plane_ref, acts_ref, out_ref):
    peers, _, _ = out_ref.shape
    width = acts_ref.shape[0] // 3
    plane = plane_ref[0]
    for peer in range(1, plane_ref.shape[0]):
        plane = plane + plane_ref[peer]
    high = plane.astype(BF16).astype(F32)
    pair = jnp.concatenate([high, plane - high], 0).astype(BF16)
    hidden = acts_ref[2 * width :]
    for peer in range(peers):
        out_ref[peer, :width] = hidden
        out_ref[peer, width:] = pair


def pert_kernel(ends_ref, gate_ref, up_ref, step_ref, radius_ref, out_ref, scale_ref, norm_ref):
    peers, _, lanes = ends_ref.shape
    width = gate_ref.shape[0]
    total = jnp.zeros((SUBLANES, lanes), F32)
    for peer in range(peers):
        pair = ends_ref[peer, width:].astype(F32)
        total = total + (pair[:SUBLANES] + pair[SUBLANES:])
    scale = radius_ref[...] * lax.rsqrt(total + 1e-06)
    norm_ref[...] = jnp.sqrt(total)
    scale_ref[...] = scale
    pgate = gate_ref[...] + scale[:1] * step_ref[:width]
    pup = up_ref[...] + scale[:1] * step_ref[width:]
    phidden = (pgate * jax.nn.sigmoid(pgate) * pup).astype(BF16)
    for peer in range(peers):
        out_ref[peer] = phidden


def out_kernel(
    core_ref, scale_ref, pt_ref, pm_ref, ht_ref, hm_ref, wd_ref, dy_ref, out_ref, ph_ref, mix_ref
):
    peers, width, half = pm_ref.shape
    part = LANES // peers

    @pl.when(pl.program_id(0) == 0)
    def _():
        for at, p_ref in ((0, pt_ref), (half, pm_ref)):
            for j in range(width // part):
                block = p_ref[:, j * part : (j + 1) * part, :].reshape(LANES, half)
                ph_ref[at : at + half, j * LANES : (j + 1) * LANES] = (
                    block.astype(F32).T.astype(BF16)
                )
        for a, p_ref in ((0, pt_ref), (half, pm_ref)):
            for b, h_ref in ((0, ht_ref), (half, hm_ref)):
                p = p_ref[...].reshape(peers * width, half)
                h = h_ref[:, :width, :].reshape(peers * width, half)
                mix = scale_ref[:1] * dot(p, h, (0, 0))
                mix_ref[a : a + half, b : b + half] = mix.astype(BF16)

    acc = dot(ph_ref[...], wd_ref[...], (1, 0)) + dot(mix_ref[...], dy_ref[...], (1, 0))
    out = acc.astype(BF16)
    theirs = pl.multiple_of((1 - core_ref[0]) * half, half)
    mine = pl.multiple_of(core_ref[0] * half, half)
    out_ref[pl.ds(theirs, half), :] = out[:half]
    out_ref[pl.ds(mine, half), :] = out[half:]


def out_terms(core, scale, ph_theirs, ph_mine, h_theirs, h_mine, w_down, dy):
    hidden, depth = w_down.shape
    tokens = dy.shape[0]
    block = min(depth, 256)
    ph_spec = pl.BlockSpec(ph_mine.shape, lambda n: (0, 0, 0))
    h_spec = pl.BlockSpec(h_mine.shape, lambda n: (0, 0, 0))
    return pl.pallas_call(
        out_kernel,
        grid=(depth // block,),
        in_specs=[
            SMEM,
            pl.BlockSpec(scale.shape, lambda n: (0, 0)),
            ph_spec,
            ph_spec,
            h_spec,
            h_spec,
            pl.BlockSpec((hidden, block), lambda n: (0, n)),
            pl.BlockSpec((tokens, block), lambda n: (0, n)),
        ],
        out_specs=pl.BlockSpec((tokens, block), lambda n: (0, n)),
        out_shape=jax.ShapeDtypeStruct((tokens, depth), BF16),
        scratch_shapes=[pltpu.VMEM((tokens, hidden), BF16), pltpu.VMEM((tokens, tokens), BF16)],
        compiler_params=pltpu.CompilerParams(vmem_limit_bytes=24 * MIB),
        cost_estimate=pl.CostEstimate(
            flops=2 * tokens * depth * hidden, bytes_accessed=2 * depth * hidden, transcendentals=0
        ),
        name="out_terms",
    )(core, scale, ph_theirs, ph_mine, h_theirs, h_mine, w_down, dy)


def per_device(tokens, grad_out, w_gate, w_up, w_down, radius):
    core = lax.axis_index(CORE).reshape(1).astype(jnp.int32)
    peers = lax.axis_size(Z)
    sources = lax.axis_size(ROW)
    rows, depth = tokens.shape
    half = sources * rows // 2
    width = w_gate.shape[1] // peers
    slab = 2 * half // peers

    radius = jnp.broadcast_to(radius, (SUBLANES, half))
    tokens, grad_out, core, radius = lax.optimization_barrier(
        (tokens, grad_out, core, radius)
    )
    fetched = exchange(copies_in(tokens, grad_out, sources), ROW)
    theirs, mine, dy = terms(core, fetched, w_gate, w_up, w_down, peers)
    arrived = swap_cores(theirs)
    chip, chip_gh = local_kernel(
        add_kernel,
        [((peers, 2 * (width + slab), half), BF16), ((peers, width, half), BF16)],
        (mine, arrived),
    )
    sums = exchange(chip, Z)
    sent, gate, up = local_kernel(
        middle_kernel,
        [
            ((peers, width + 2 * slab, half), BF16),
            ((width, half), F32),
            ((width, half), F32),
        ],
        (sums, chip_gh),
    )
    sums = exchange(sent, Z)
    (acts,) = local_kernel(acts_kernel, [((3 * width, half), BF16)], (sums, gate, up))
    arrived = swap_cores(acts)
    step, local = local_kernel(
        step_kernel,
        [((2 * width, half), F32), ((2 * sources, SUBLANES, LANES), F32)],
        (core, acts, arrived, sums),
    )
    plane = exchange(local, (*ROW, CORE))
    (sent,) = local_kernel(
        norm_kernel, [((peers, width + 2 * SUBLANES, half), BF16)], (plane, acts)
    )
    h_mine = exchange(sent, Z)
    tile = ((SUBLANES, half), F32)
    sent, scale, norm = local_kernel(
        pert_kernel, [((peers, width, half), BF16), tile, tile], (h_mine, gate, up, step, radius)
    )
    ph_mine = exchange(sent, Z)
    ph_mine, h_mine = lax.optimization_barrier((ph_mine, h_mine))
    ph_theirs = swap_cores(ph_mine)
    h_theirs = swap_cores(h_mine)
    partial_out = out_terms(core, scale, ph_theirs, ph_mine, h_theirs, h_mine, w_down, dy)
    partial_out, norm = lax.optimization_barrier((partial_out, norm[0, :1]))
    parts = exchange(partial_out.reshape(sources, rows, depth), ROW)
    return (jnp.sum(parts.astype(F32), 0).astype(BF16), norm)


TERMS_MIB = 60


def solution(mesh):
    split = Mesh(mesh.devices.reshape(4, 4, 8, 2), ("row_0", "row_1", "col_0", "col_1"))
    return jax.shard_map(
        per_device,
        mesh=split,
        in_specs=(P(ROW, COL), P(ROW, COL), P(COL, ROW), P(COL, ROW), P(ROW, COL), P()),
        out_specs=(P(ROW, COL), P()),
        check_vma=False,
    )
```

```python
import jax
import jax.numpy as jnp
from jax import lax
from jax.experimental import pallas as pl
from jax.experimental.pallas import tpu as pltpu
from jax.sharding import Mesh
from jax.sharding import PartitionSpec as P

ROW = ("row_0", "row_1")
COL = ("col_0", "col_1")
Z = "col_0"
CORE = "col_1"
F32 = jnp.float32
BF16 = jnp.bfloat16
LANES = 128
SUBLANES = 8
MIB = 1 << 20
VMEM = pl.BlockSpec(memory_space=pltpu.VMEM)
SMEM = pl.BlockSpec(memory_space=pltpu.SMEM)


def dot(left, right, over):
    return lax.dot_general(
        left, right, (((over[0],), (over[1],)), ((), ())), preferred_element_type=F32
    )


def exchange(x, axis):
    return lax.all_to_all(x, axis, 0, 0, tiled=True)


def swap_cores(x):
    return lax.ppermute(x, CORE, [(0, 1), (1, 0)])


def local_kernel(body, out_shape, operands, limit=16, flops=1_000_000):
    return pl.pallas_call(
        body,
        in_specs=[SMEM if a.dtype == jnp.int32 else VMEM for a in operands],
        out_specs=[VMEM] * len(out_shape),
        out_shape=[jax.ShapeDtypeStruct(*shape) for shape in out_shape],
        compiler_params=pltpu.CompilerParams(vmem_limit_bytes=limit * MIB),
        cost_estimate=pl.CostEstimate(flops=flops, bytes_accessed=1_000_000, transcendentals=0),
    )(*operands)


def copies_in_kernel(tokens_ref, dy_ref, out_ref, done):
    rows = tokens_ref.shape[0]
    copies = [
        pltpu.make_async_copy(
            own_ref, out_ref.at[0, kind * rows : (kind + 1) * rows], done.at[kind]
        )
        for kind, own_ref in enumerate((tokens_ref, dy_ref))
    ]
    for copy in copies:
        copy.start()
    for copy in copies:
        copy.wait()
    both = out_ref[0]
    for peer in range(1, out_ref.shape[0]):
        out_ref[peer] = both


def copies_in(tokens, grad_out, sources):
    rows, depth = tokens.shape
    return pl.pallas_call(
        copies_in_kernel,
        in_specs=[pl.BlockSpec(memory_space=pl.ANY)] * 2,
        out_specs=VMEM,
        out_shape=jax.ShapeDtypeStruct((sources, 2 * rows, depth), BF16),
        scratch_shapes=[pltpu.SemaphoreType.DMA((2,))],
        compiler_params=pltpu.CompilerParams(vmem_limit_bytes=4 * MIB),
        cost_estimate=pl.CostEstimate(flops=20_000_000_000, bytes_accessed=1_000_000, transcendentals=0),
        name="copies_in",
    )(tokens, grad_out)


def terms_kernel(
    place_ref, in_ref, wg_ref, wu_ref, wd_ref, theirs_ref, mine_ref, ord_ref, prod_ref
):
    j = pl.program_id(0)
    steps = wg_ref.shape[1] // LANES
    peers = theirs_ref.shape[0]
    sources, rows2, depth = in_ref.shape
    rows = rows2 // 2
    tokens = sources * rows
    half = tokens // 2
    slab = tokens // peers
    part = LANES // peers
    width = steps * part
    core = place_ref[0]
    sides = ((1 - core, theirs_ref), (core, mine_ref))

    @pl.when(j == 0)
    def _():
        for kind in range(2):
            row_at = 2 * width + kind * slab
            a = in_ref[:, kind * rows : (kind + 1) * rows, :].reshape(tokens, depth)
            for side, out_ref in sides:
                own = in_ref[
                    pl.ds(side * (sources // 2), sources // 2), kind * rows : (kind + 1) * rows, :
                ].reshape(half, depth)
                gram = dot(a, own, (1, 1)).astype(BF16)
                out_ref[:, row_at : row_at + slab, :] = gram.reshape(peers, slab, half)
        for at, side in ((0, 1 - core), (half, core)):
            own = in_ref[pl.ds(side * (sources // 2), sources // 2), rows:, :]
            ord_ref[at : at + half] = own.reshape(half, depth)

    last = pl.multiple_of(jnp.maximum(j - 1, 0) * part, part)
    for side, out_ref in sides:
        token_at = pl.multiple_of(side * half, half)
        block = prod_ref[lax.rem(j + 1, 2), pl.ds(token_at, half), :].T.astype(BF16)
        out_ref[:, pl.ds(last, part), :] = block[:LANES].reshape(peers, part, half)
        out_ref[:, pl.ds(width + last, part), :] = block[LANES:].reshape(peers, part, half)
    x = in_ref[:, :rows, :].reshape(tokens, depth)
    now = pl.multiple_of(jnp.minimum(j, steps - 1) * LANES, LANES)
    w = jnp.concatenate([wg_ref[:, pl.ds(now, LANES)], wu_ref[:, pl.ds(now, LANES)]], 1)
    prod_ref[lax.rem(j, 2)] = jnp.dot(x, w, preferred_element_type=F32)

    @pl.when(j == steps)
    def _():
        for first in range(0, steps, 4):
            end = min(first + 4, steps)
            rows_in = slice(first * LANES, end * LANES)
            block = dot(wd_ref[rows_in], ord_ref[...], (1, 1)).astype(BF16)
            for step in range(first, end):
                piece = block[(step - first) * LANES : (step - first + 1) * LANES]
                piece = piece.reshape(peers, part, tokens)
                to = 2 * width + 2 * slab + step * part
                theirs_ref[:, to : to + part, :] = piece[:, :, :half]
                mine_ref[:, to : to + part, :] = piece[:, :, half:]


def terms(place, fetched, w_gate, w_up, w_down, peers):
    depth, hidden = w_gate.shape
    tokens = fetched.shape[0] * fetched.shape[1] // 2
    steps = hidden // LANES
    rows = 3 * hidden // peers + 2 * tokens // peers
    out = jax.ShapeDtypeStruct((peers, rows, tokens // 2), BF16)
    dy = jax.ShapeDtypeStruct((tokens, depth), BF16)
    return pl.pallas_call(
        terms_kernel,
        grid=(steps + 1,),
        in_specs=[SMEM] + [VMEM] * 4,
        out_specs=[VMEM] * 3,
        out_shape=[out, out, dy],
        scratch_shapes=[pltpu.VMEM((2, tokens, 2 * LANES), F32)],
        compiler_params=pltpu.CompilerParams(vmem_limit_bytes=TERMS_MIB * MIB),
        cost_estimate=pl.CostEstimate(
            flops=6 * tokens * depth * hidden, bytes_accessed=6 * depth * hidden, transcendentals=0
        ),
        name="terms",
    )(place, fetched, w_gate, w_up, w_down)


def split_kernel(place_ref, mine_ref, arrived_ref, first_ref, second_ref, keep_ref):
    parity = lax.rem(place_ref[1], 2)
    cut = first_ref.shape[1]
    for q in range(keep_ref.shape[0]):
        away, here = 2 * q + 1 - parity, 2 * q + parity
        sent = (mine_ref[away].astype(F32) + arrived_ref[away].astype(F32)).astype(BF16)
        first_ref[q] = sent[:cut]
        second_ref[q] = sent[cut:]
        keep_ref[q] = mine_ref[here].astype(F32) + arrived_ref[here].astype(F32)


def pair_kernel(place_ref, keep_ref, first_ref, second_ref, own_ref, up_ref, down_ref, far_ref):
    count = keep_ref.shape[0]
    cut = first_ref.shape[1]
    q0 = place_ref[1] // 2
    for shift, out_ref in ((0, own_ref), (1, up_ref), (count - 1, down_ref), (2, far_ref)):
        q = lax.rem(q0 + shift, count)
        out_ref[:cut] = (keep_ref[q, :cut] + first_ref[q].astype(F32)).astype(out_ref.dtype)
        out_ref[cut:] = (keep_ref[q, cut:] + second_ref[q].astype(F32)).astype(out_ref.dtype)


def acts_kernel(own_ref, up_in, down_in, far_in, gate_ref, up_ref, acts_ref, grams_ref):
    width = gate_ref.shape[0]
    peers, slabs, _ = grams_ref.shape
    total = own_ref[...] + up_in[...].astype(F32)
    total = total + down_in[...].astype(F32) + far_in[...].astype(F32)
    gate, up = total[:width], total[width : 2 * width]
    grams = total[2 * width : 2 * width + slabs].astype(BF16)
    grad_hidden = total[2 * width + slabs :].astype(BF16).astype(F32)
    sig = jax.nn.sigmoid(gate)
    silu = gate * sig
    gate_ref[...] = gate
    up_ref[...] = up
    acts_ref[:width] = (grad_hidden * up * sig * (1.0 + gate * (1.0 - sig))).astype(BF16)
    acts_ref[width : 2 * width] = (grad_hidden * silu).astype(BF16)
    acts_ref[2 * width :] = (silu * up).astype(BF16)
    for peer in range(peers):
        grams_ref[peer] = grams


def step_kernel(place_ref, acts_ref, arrived_ref, grams_ref, step_ref, local_ref):
    peers, rows, half = grams_ref.shape
    width = acts_ref.shape[0] // 3
    slab = rows // 2
    core = place_ref[0]
    kinds = ((0, 2 * width, 0), (2 * width, 3 * width, slab))
    local = 0.0
    for first, end, at in kinds:
        product = 0.0
        for side, part_ref in ((1 - core, arrived_ref), (core, acts_ref)):
            gram = grams_ref[pl.ds(side * (peers // 2), peers // 2), at : at + slab, :]
            product += dot(part_ref[first:end], gram.reshape(half, half), (1, 0))
        local += jnp.sum(acts_ref[first:end].astype(F32) * product)
        if first == 0:
            step_ref[...] = product
    local_ref[...] = jnp.full(local_ref.shape, local, F32)


def norm_kernel(plane_ref, acts_ref, out_ref):
    peers, _, _ = out_ref.shape
    width = acts_ref.shape[0] // 3
    plane = plane_ref[0]
    for peer in range(1, plane_ref.shape[0]):
        plane = plane + plane_ref[peer]
    high = plane.astype(BF16).astype(F32)
    pair = jnp.concatenate([high, plane - high], 0).astype(BF16)
    hidden = acts_ref[2 * width :]
    for peer in range(peers):
        out_ref[peer, :width] = hidden
        out_ref[peer, width:] = pair


def pert_kernel(ends_ref, gate_ref, up_ref, step_ref, radius_ref, out_ref, scale_ref, norm_ref):
    peers, _, lanes = ends_ref.shape
    width = gate_ref.shape[0]
    total = jnp.zeros((SUBLANES, lanes), F32)
    for peer in range(peers):
        pair = ends_ref[peer, width:].astype(F32)
        total = total + (pair[:SUBLANES] + pair[SUBLANES:])
    scale = radius_ref[...] * lax.rsqrt(total + 1e-06)
    norm_ref[...] = jnp.sqrt(total)
    scale_ref[...] = scale
    pgate = gate_ref[...] + scale[:1] * step_ref[:width]
    pup = up_ref[...] + scale[:1] * step_ref[width:]
    phidden = (pgate * jax.nn.sigmoid(pgate) * pup).astype(BF16)
    for peer in range(peers):
        out_ref[peer] = phidden


def out_kernel(
    place_ref, scale_ref, pt_ref, pm_ref, ht_ref, hm_ref, wd_ref, dy_ref, out_ref, ph_ref, mix_ref
):
    peers, width, half = pm_ref.shape
    part = LANES // peers

    @pl.when(pl.program_id(0) == 0)
    def _():
        for at, p_ref in ((0, pt_ref), (half, pm_ref)):
            for j in range(width // part):
                block = p_ref[:, j * part : (j + 1) * part, :].reshape(LANES, half)
                ph_ref[at : at + half, j * LANES : (j + 1) * LANES] = (
                    block.astype(F32).T.astype(BF16)
                )
        for a, p_ref in ((0, pt_ref), (half, pm_ref)):
            for b, h_ref in ((0, ht_ref), (half, hm_ref)):
                p = p_ref[...].reshape(peers * width, half)
                h = h_ref[:, :width, :].reshape(peers * width, half)
                mix = scale_ref[:1] * dot(p, h, (0, 0))
                mix_ref[a : a + half, b : b + half] = mix.astype(BF16)

    acc = dot(ph_ref[...], wd_ref[...], (1, 0)) + dot(mix_ref[...], dy_ref[...], (1, 0))
    out = acc.astype(BF16)
    theirs = pl.multiple_of((1 - place_ref[0]) * half, half)
    mine = pl.multiple_of(place_ref[0] * half, half)
    out_ref[pl.ds(theirs, half), :] = out[:half]
    out_ref[pl.ds(mine, half), :] = out[half:]


def out_terms(place, scale, ph_theirs, ph_mine, h_theirs, h_mine, w_down, dy):
    hidden, depth = w_down.shape
    tokens = dy.shape[0]
    block = min(depth, 256)
    ph_spec = pl.BlockSpec(ph_mine.shape, lambda n: (0, 0, 0))
    h_spec = pl.BlockSpec(h_mine.shape, lambda n: (0, 0, 0))
    return pl.pallas_call(
        out_kernel,
        grid=(depth // block,),
        in_specs=[
            SMEM,
            pl.BlockSpec(scale.shape, lambda n: (0, 0)),
            ph_spec,
            ph_spec,
            h_spec,
            h_spec,
            pl.BlockSpec((hidden, block), lambda n: (0, n)),
            pl.BlockSpec((tokens, block), lambda n: (0, n)),
        ],
        out_specs=pl.BlockSpec((tokens, block), lambda n: (0, n)),
        out_shape=jax.ShapeDtypeStruct((tokens, depth), BF16),
        scratch_shapes=[pltpu.VMEM((tokens, hidden), BF16), pltpu.VMEM((tokens, tokens), BF16)],
        compiler_params=pltpu.CompilerParams(vmem_limit_bytes=24 * MIB),
        cost_estimate=pl.CostEstimate(
            flops=2 * tokens * depth * hidden, bytes_accessed=2 * depth * hidden, transcendentals=0
        ),
        name="out_terms",
    )(place, scale, ph_theirs, ph_mine, h_theirs, h_mine, w_down, dy)


def per_device(tokens, grad_out, w_gate, w_up, w_down, radius):
    peers = lax.axis_size(Z)
    sources = lax.axis_size(ROW)
    rows, depth = tokens.shape
    half = sources * rows // 2
    width = w_gate.shape[1] // peers
    slab = 2 * half // peers
    every = 3 * width + 2 * slab
    cut = (every + 31) // 32 * 16
    neighbour = [(z, z ^ 1) for z in range(peers)]
    other = [(z, (z + 2 * (z % 2) - 1) % peers) for z in range(peers)]

    def moved(x, by):
        return lax.ppermute(x, Z, [(z, (z + by) % peers) for z in range(peers)])

    radius = jnp.broadcast_to(radius, (SUBLANES, half))
    place = jnp.stack([lax.axis_index(CORE), lax.axis_index(Z)]).astype(jnp.int32)
    tokens, grad_out, place, radius = lax.optimization_barrier((tokens, grad_out, place, radius))
    fetched = exchange(copies_in(tokens, grad_out, sources), ROW)
    theirs, mine, dy = terms(place, fetched, w_gate, w_up, w_down, peers)
    arrived = swap_cores(theirs)
    first, second, keep = local_kernel(
        split_kernel,
        [
            ((peers // 2, cut, half), BF16),
            ((peers // 2, every - cut, half), BF16),
            ((peers // 2, every, half), F32),
        ],
        (place, mine, arrived),
    )
    first = lax.ppermute(first, Z, neighbour)
    second = lax.ppermute(second, Z, other)
    block = ((every, half), BF16)
    own, up_block, down_block, far_block = local_kernel(
        pair_kernel, [((every, half), F32), block, block, block], (place, keep, first, second)
    )
    blocks = (moved(up_block, 2), moved(down_block, -2), moved(far_block, 4))
    gate, up, acts, grams = local_kernel(
        acts_kernel,
        [
            ((width, half), F32),
            ((width, half), F32),
            ((3 * width, half), BF16),
            ((peers, 2 * slab, half), BF16),
        ],
        (own, *blocks),
    )
    arrived = swap_cores(acts)
    arrived, grams = lax.optimization_barrier((arrived, grams))
    sums = exchange(grams, Z)
    step, local = local_kernel(
        step_kernel,
        [((2 * width, half), F32), ((2 * sources, SUBLANES, LANES), F32)],
        (place, acts, arrived, sums),
    )
    plane = exchange(local, (*ROW, CORE))
    (sent,) = local_kernel(
        norm_kernel, [((peers, width + 2 * SUBLANES, half), BF16)], (plane, acts)
    )
    h_mine = exchange(sent, Z)
    tile = ((SUBLANES, half), F32)
    sent, scale, norm = local_kernel(
        pert_kernel, [((peers, width, half), BF16), tile, tile], (h_mine, gate, up, step, radius)
    )
    ph_mine = exchange(sent, Z)
    ph_mine, h_mine = lax.optimization_barrier((ph_mine, h_mine))
    ph_theirs = swap_cores(ph_mine)
    h_theirs = swap_cores(h_mine)
    partial_out = out_terms(place, scale, ph_theirs, ph_mine, h_theirs, h_mine, w_down, dy)
    partial_out, norm = lax.optimization_barrier((partial_out, norm[0, :1]))
    parts = exchange(partial_out.reshape(sources, rows, depth), ROW)
    return (jnp.sum(parts.astype(F32), 0).astype(BF16), norm)


TERMS_MIB = 24


def solution(mesh):
    split = Mesh(mesh.devices.reshape(4, 4, 8, 2), ("row_0", "row_1", "col_0", "col_1"))
    return jax.shard_map(
        per_device,
        mesh=split,
        in_specs=(P(ROW, COL), P(ROW, COL), P(COL, ROW), P(COL, ROW), P(ROW, COL), P()),
        out_specs=(P(ROW, COL), P()),
        check_vma=False,
    )
```

```python
import jax
import jax.numpy as jnp
from jax import lax
from jax.experimental import pallas as pl
from jax.experimental.pallas import tpu as pltpu
from jax.sharding import Mesh
from jax.sharding import PartitionSpec as P

ROW = ("row_0", "row_1")
COL = ("col_0", "col_1")
Z = "col_0"
CORE = "col_1"
F32 = jnp.float32
BF16 = jnp.bfloat16
LANES = 128
SUBLANES = 8
MIB = 1 << 20
VMEM = pl.BlockSpec(memory_space=pltpu.VMEM)
SMEM = pl.BlockSpec(memory_space=pltpu.SMEM)


def dot(left, right, over):
    return lax.dot_general(
        left, right, (((over[0],), (over[1],)), ((), ())), preferred_element_type=F32
    )


def exchange(x, axis):
    return lax.all_to_all(x, axis, 0, 0, tiled=True)


def swap_cores(x):
    return lax.ppermute(x, CORE, [(0, 1), (1, 0)])


def local_kernel(body, out_shape, operands, limit=16, flops=1_000_000):
    return pl.pallas_call(
        body,
        in_specs=[SMEM if a.dtype == jnp.int32 else VMEM for a in operands],
        out_specs=[VMEM] * len(out_shape),
        out_shape=[jax.ShapeDtypeStruct(*shape) for shape in out_shape],
        compiler_params=pltpu.CompilerParams(vmem_limit_bytes=limit * MIB),
        cost_estimate=pl.CostEstimate(flops=flops, bytes_accessed=1_000_000, transcendentals=0),
    )(*operands)


def copies_in_kernel(tokens_ref, dy_ref, out_ref, done):
    rows = tokens_ref.shape[0]
    copies = [
        pltpu.make_async_copy(
            own_ref, out_ref.at[0, kind * rows : (kind + 1) * rows], done.at[kind]
        )
        for kind, own_ref in enumerate((tokens_ref, dy_ref))
    ]
    for copy in copies:
        copy.start()
    for copy in copies:
        copy.wait()
    both = out_ref[0]
    for peer in range(1, out_ref.shape[0]):
        out_ref[peer] = both


def copies_in(tokens, grad_out, sources):
    rows, depth = tokens.shape
    return pl.pallas_call(
        copies_in_kernel,
        in_specs=[pl.BlockSpec(memory_space=pl.ANY)] * 2,
        out_specs=VMEM,
        out_shape=jax.ShapeDtypeStruct((sources, 2 * rows, depth), BF16),
        scratch_shapes=[pltpu.SemaphoreType.DMA((2,))],
        compiler_params=pltpu.CompilerParams(vmem_limit_bytes=4 * MIB),
        cost_estimate=pl.CostEstimate(flops=20_000_000_000, bytes_accessed=1_000_000, transcendentals=0),
        name="copies_in",
    )(tokens, grad_out)


def terms_kernel(
    place_ref, in_ref, wg_ref, wu_ref, wd_ref, theirs_ref, mine_ref, ord_ref, prod_ref
):
    j = pl.program_id(0)
    steps = wg_ref.shape[1] // LANES
    peers = theirs_ref.shape[0]
    sources, rows2, depth = in_ref.shape
    rows = rows2 // 2
    tokens = sources * rows
    half = tokens // 2
    part = LANES // peers
    width = steps * part
    core = place_ref[0]
    sides = ((1 - core, theirs_ref), (core, mine_ref))

    @pl.when(j == 0)
    def _():
        for at, side in ((0, 1 - core), (half, core)):
            own = in_ref[pl.ds(side * (sources // 2), sources // 2), rows:, :]
            ord_ref[at : at + half] = own.reshape(half, depth)

    last = pl.multiple_of(jnp.maximum(j - 1, 0) * part, part)
    for side, out_ref in sides:
        token_at = pl.multiple_of(side * half, half)
        block = prod_ref[lax.rem(j + 1, 2), pl.ds(token_at, half), :].T.astype(BF16)
        out_ref[:, pl.ds(last, part), :] = block[:LANES].reshape(peers, part, half)
        out_ref[:, pl.ds(width + last, part), :] = block[LANES:].reshape(peers, part, half)
    x = in_ref[:, :rows, :].reshape(tokens, depth)
    now = pl.multiple_of(jnp.minimum(j, steps - 1) * LANES, LANES)
    w = jnp.concatenate([wg_ref[:, pl.ds(now, LANES)], wu_ref[:, pl.ds(now, LANES)]], 1)
    prod_ref[lax.rem(j, 2)] = jnp.dot(x, w, preferred_element_type=F32)

    @pl.when(j == steps)
    def _():
        for first in range(0, steps, 4):
            end = min(first + 4, steps)
            rows_in = slice(first * LANES, end * LANES)
            block = dot(wd_ref[rows_in], ord_ref[...], (1, 1)).astype(BF16)
            for step in range(first, end):
                piece = block[(step - first) * LANES : (step - first + 1) * LANES]
                piece = piece.reshape(peers, part, tokens)
                to = 2 * width + step * part
                theirs_ref[:, to : to + part, :] = piece[:, :, :half]
                mine_ref[:, to : to + part, :] = piece[:, :, half:]


def terms(place, fetched, w_gate, w_up, w_down, peers):
    depth, hidden = w_gate.shape
    tokens = fetched.shape[0] * fetched.shape[1] // 2
    steps = hidden // LANES
    rows = 3 * hidden // peers
    out = jax.ShapeDtypeStruct((peers, rows, tokens // 2), BF16)
    dy = jax.ShapeDtypeStruct((tokens, depth), BF16)
    return pl.pallas_call(
        terms_kernel,
        grid=(steps + 1,),
        in_specs=[SMEM] + [VMEM] * 4,
        out_specs=[VMEM] * 3,
        out_shape=[out, out, dy],
        scratch_shapes=[pltpu.VMEM((2, tokens, 2 * LANES), F32)],
        compiler_params=pltpu.CompilerParams(vmem_limit_bytes=TERMS_MIB * MIB),
        cost_estimate=pl.CostEstimate(
            flops=6 * tokens * depth * hidden, bytes_accessed=6 * depth * hidden, transcendentals=0
        ),
        name="terms",
    )(place, fetched, w_gate, w_up, w_down)


def gram_kernel(place_ref, in_ref, theirs_ref, mine_ref):
    sources, rows2, depth = in_ref.shape
    rows = rows2 // 2
    half = sources * rows // 2
    core, row = place_ref[0], place_ref[2]
    for side, out_ref in ((1 - core, theirs_ref), (core, mine_ref)):
        for kind in range(2):
            at = slice(kind * rows, (kind + 1) * rows)
            every = in_ref[pl.ds(side * (sources // 2), sources // 2), at, :]
            out_ref[at] = dot(in_ref[row, at], every.reshape(half, depth), (1, 1)).astype(BF16)


def gram_sum_kernel(*refs):
    *terms_in, out_ref = refs
    total = terms_in[0][...].astype(F32)
    for ref in terms_in[1:]:
        total = total + ref[...].astype(F32)
    total = total.astype(BF16)
    if len(out_ref.shape) == 2:
        out_ref[...] = total
    else:
        for peer in range(out_ref.shape[0]):
            out_ref[peer] = total


def gram_table_kernel(parts_ref, table_ref):
    sources, rows2, half = parts_ref.shape
    rows = rows2 // 2
    for kind in range(2):
        part = parts_ref[:, kind * rows : (kind + 1) * rows, :]
        table_ref[kind] = part.reshape(sources * rows, half)


def split_kernel(place_ref, mine_ref, arrived_ref, first_ref, second_ref, keep_ref):
    parity = lax.rem(place_ref[1], 2)
    cut = first_ref.shape[1]
    for q in range(keep_ref.shape[0]):
        away, here = 2 * q + 1 - parity, 2 * q + parity
        sent = (mine_ref[away].astype(F32) + arrived_ref[away].astype(F32)).astype(BF16)
        first_ref[q] = sent[:cut]
        second_ref[q] = sent[cut:]
        keep_ref[q] = mine_ref[here].astype(F32) + arrived_ref[here].astype(F32)


def pair_kernel(place_ref, keep_ref, first_ref, second_ref, own_ref, up_ref, down_ref, far_ref):
    count = keep_ref.shape[0]
    cut = first_ref.shape[1]
    q0 = place_ref[1] // 2
    for shift, out_ref in ((0, own_ref), (1, up_ref), (count - 1, down_ref), (2, far_ref)):
        q = lax.rem(q0 + shift, count)
        out_ref[:cut] = (keep_ref[q, :cut] + first_ref[q].astype(F32)).astype(out_ref.dtype)
        out_ref[cut:] = (keep_ref[q, cut:] + second_ref[q].astype(F32)).astype(out_ref.dtype)


def acts_kernel(own_ref, up_in, down_in, far_in, gate_ref, up_ref, acts_ref):
    width = gate_ref.shape[0]
    total = own_ref[...] + up_in[...].astype(F32)
    total = total + down_in[...].astype(F32) + far_in[...].astype(F32)
    gate, up = total[:width], total[width : 2 * width]
    grad_hidden = total[2 * width :].astype(BF16).astype(F32)
    sig = jax.nn.sigmoid(gate)
    silu = gate * sig
    gate_ref[...] = gate
    up_ref[...] = up
    acts_ref[:width] = (grad_hidden * up * sig * (1.0 + gate * (1.0 - sig))).astype(BF16)
    acts_ref[width : 2 * width] = (grad_hidden * silu).astype(BF16)
    acts_ref[2 * width :] = (silu * up).astype(BF16)


def step_kernel(place_ref, acts_ref, arrived_ref, grams_ref, step_ref, local_ref):
    half = grams_ref.shape[2]
    width = acts_ref.shape[0] // 3
    core = place_ref[0]
    kinds = ((0, 2 * width, 0), (2 * width, 3 * width, 1))
    local = 0.0
    for first, end, kind in kinds:
        product = 0.0
        for side, part_ref in ((1 - core, arrived_ref), (core, acts_ref)):
            gram = grams_ref[kind, pl.ds(pl.multiple_of(side * half, half), half), :]
            product += dot(part_ref[first:end], gram, (1, 0))
        local += jnp.sum(acts_ref[first:end].astype(F32) * product)
        if first == 0:
            step_ref[...] = product
    local_ref[...] = jnp.full(local_ref.shape, local, F32)


def norm_kernel(plane_ref, acts_ref, out_ref):
    peers, _, _ = out_ref.shape
    width = acts_ref.shape[0] // 3
    plane = plane_ref[0]
    for peer in range(1, plane_ref.shape[0]):
        plane = plane + plane_ref[peer]
    high = plane.astype(BF16).astype(F32)
    pair = jnp.concatenate([high, plane - high], 0).astype(BF16)
    hidden = acts_ref[2 * width :]
    for peer in range(peers):
        out_ref[peer, :width] = hidden
        out_ref[peer, width:] = pair


def pert_kernel(ends_ref, gate_ref, up_ref, step_ref, radius_ref, out_ref, scale_ref, norm_ref):
    peers, _, lanes = ends_ref.shape
    width = gate_ref.shape[0]
    total = jnp.zeros((SUBLANES, lanes), F32)
    for peer in range(peers):
        pair = ends_ref[peer, width:].astype(F32)
        total = total + (pair[:SUBLANES] + pair[SUBLANES:])
    scale = radius_ref[...] * lax.rsqrt(total + 1e-06)
    norm_ref[...] = jnp.sqrt(total)
    scale_ref[...] = scale
    pgate = gate_ref[...] + scale[:1] * step_ref[:width]
    pup = up_ref[...] + scale[:1] * step_ref[width:]
    phidden = (pgate * jax.nn.sigmoid(pgate) * pup).astype(BF16)
    for peer in range(peers):
        out_ref[peer] = phidden


def out_kernel(
    place_ref, scale_ref, pt_ref, pm_ref, ht_ref, hm_ref, wd_ref, dy_ref, out_ref, ph_ref, mix_ref
):
    peers, width, half = pm_ref.shape
    part = LANES // peers

    @pl.when(pl.program_id(0) == 0)
    def _():
        for at, p_ref in ((0, pt_ref), (half, pm_ref)):
            for j in range(width // part):
                block = p_ref[:, j * part : (j + 1) * part, :].reshape(LANES, half)
                ph_ref[at : at + half, j * LANES : (j + 1) * LANES] = (
                    block.astype(F32).T.astype(BF16)
                )
        for a, p_ref in ((0, pt_ref), (half, pm_ref)):
            for b, h_ref in ((0, ht_ref), (half, hm_ref)):
                p = p_ref[...].reshape(peers * width, half)
                h = h_ref[:, :width, :].reshape(peers * width, half)
                mix = scale_ref[:1] * dot(p, h, (0, 0))
                mix_ref[a : a + half, b : b + half] = mix.astype(BF16)

    acc = dot(ph_ref[...], wd_ref[...], (1, 0)) + dot(mix_ref[...], dy_ref[...], (1, 0))
    out = acc.astype(BF16)
    theirs = pl.multiple_of((1 - place_ref[0]) * half, half)
    mine = pl.multiple_of(place_ref[0] * half, half)
    out_ref[pl.ds(theirs, half), :] = out[:half]
    out_ref[pl.ds(mine, half), :] = out[half:]


def out_terms(place, scale, ph_theirs, ph_mine, h_theirs, h_mine, w_down, dy):
    hidden, depth = w_down.shape
    tokens = dy.shape[0]
    block = min(depth, 256)
    ph_spec = pl.BlockSpec(ph_mine.shape, lambda n: (0, 0, 0))
    h_spec = pl.BlockSpec(h_mine.shape, lambda n: (0, 0, 0))
    return pl.pallas_call(
        out_kernel,
        grid=(depth // block,),
        in_specs=[
            SMEM,
            pl.BlockSpec(scale.shape, lambda n: (0, 0)),
            ph_spec,
            ph_spec,
            h_spec,
            h_spec,
            pl.BlockSpec((hidden, block), lambda n: (0, n)),
            pl.BlockSpec((tokens, block), lambda n: (0, n)),
        ],
        out_specs=pl.BlockSpec((tokens, block), lambda n: (0, n)),
        out_shape=jax.ShapeDtypeStruct((tokens, depth), BF16),
        scratch_shapes=[pltpu.VMEM((tokens, hidden), BF16), pltpu.VMEM((tokens, tokens), BF16)],
        compiler_params=pltpu.CompilerParams(vmem_limit_bytes=24 * MIB),
        cost_estimate=pl.CostEstimate(
            flops=2 * tokens * depth * hidden, bytes_accessed=2 * depth * hidden, transcendentals=0
        ),
        name="out_terms",
    )(place, scale, ph_theirs, ph_mine, h_theirs, h_mine, w_down, dy)


def per_device(tokens, grad_out, w_gate, w_up, w_down, radius):
    peers = lax.axis_size(Z)
    sources = lax.axis_size(ROW)
    rows, depth = tokens.shape
    half = sources * rows // 2
    width = w_gate.shape[1] // peers
    every = 3 * width
    cut = (every + 31) // 32 * 16
    neighbour = [(z, z ^ 1) for z in range(peers)]
    other = [(z, (z + 2 * (z % 2) - 1) % peers) for z in range(peers)]

    def moved(x, by):
        return lax.ppermute(x, Z, [(z, (z + by) % peers) for z in range(peers)])

    radius = jnp.broadcast_to(radius, (SUBLANES, half))
    place = jnp.stack([lax.axis_index(axis) for axis in (CORE, Z, ROW)]).astype(jnp.int32)
    tokens, grad_out, place, radius = lax.optimization_barrier((tokens, grad_out, place, radius))
    fetched = exchange(copies_in(tokens, grad_out, sources), ROW)
    flat = ((2 * rows, half), BF16)
    theirs, gram = local_kernel(gram_kernel, [flat, flat], (place, fetched))
    fetched, theirs = lax.optimization_barrier((fetched, theirs))
    theirs = swap_cores(theirs)
    theirs_wide, mine, dy = terms(place, fetched, w_gate, w_up, w_down, peers)
    (gram,) = local_kernel(gram_sum_kernel, [flat], (gram, theirs))
    theirs_wide, gram = lax.optimization_barrier((theirs_wide, gram))
    arrived = swap_cores(theirs_wide)
    theirs = lax.ppermute(gram, Z, neighbour)
    (gram,) = local_kernel(gram_sum_kernel, [flat], (gram, theirs))
    first, second, keep = local_kernel(
        split_kernel,
        [
            ((peers // 2, cut, half), BF16),
            ((peers // 2, every - cut, half), BF16),
            ((peers // 2, every, half), F32),
        ],
        (place, mine, arrived),
    )
    first = lax.ppermute(first, Z, neighbour)
    second = lax.ppermute(second, Z, other)
    others = (moved(gram, 2), moved(gram, -2), moved(gram, 4))
    (grams,) = local_kernel(gram_sum_kernel, [((sources, 2 * rows, half), BF16)], (gram, *others))
    block = ((every, half), BF16)
    own, up_block, down_block, far_block = local_kernel(
        pair_kernel, [((every, half), F32), block, block, block], (place, keep, first, second)
    )
    blocks = (moved(up_block, 2), moved(down_block, -2), moved(far_block, 4))
    grams = exchange(grams, ROW)
    (sums,) = local_kernel(gram_table_kernel, [((2, 2 * half, half), BF16)], (grams,))
    gate, up, acts = local_kernel(
        acts_kernel,
        [
            ((width, half), F32),
            ((width, half), F32),
            ((3 * width, half), BF16),
        ],
        (own, *blocks),
    )
    arrived = swap_cores(acts)
    step, local = local_kernel(
        step_kernel,
        [((2 * width, half), F32), ((2 * sources, SUBLANES, LANES), F32)],
        (place, acts, arrived, sums),
    )
    plane = exchange(local, (*ROW, CORE))
    (sent,) = local_kernel(
        norm_kernel, [((peers, width + 2 * SUBLANES, half), BF16)], (plane, acts)
    )
    h_mine = exchange(sent, Z)
    tile = ((SUBLANES, half), F32)
    sent, scale, norm = local_kernel(
        pert_kernel, [((peers, width, half), BF16), tile, tile], (h_mine, gate, up, step, radius)
    )
    ph_mine = exchange(sent, Z)
    ph_mine, h_mine = lax.optimization_barrier((ph_mine, h_mine))
    ph_theirs = swap_cores(ph_mine)
    h_theirs = swap_cores(h_mine)
    partial_out = out_terms(place, scale, ph_theirs, ph_mine, h_theirs, h_mine, w_down, dy)
    partial_out, norm = lax.optimization_barrier((partial_out, norm[0, :1]))
    parts = exchange(partial_out.reshape(sources, rows, depth), ROW)
    return (jnp.sum(parts.astype(F32), 0).astype(BF16), norm)


TERMS_MIB = 24


def solution(mesh):
    split = Mesh(mesh.devices.reshape(4, 4, 8, 2), ("row_0", "row_1", "col_0", "col_1"))
    return jax.shard_map(
        per_device,
        mesh=split,
        in_specs=(P(ROW, COL), P(ROW, COL), P(COL, ROW), P(COL, ROW), P(ROW, COL), P()),
        out_specs=(P(ROW, COL), P()),
        check_vma=False,
    )
```

```python
import jax
import jax.numpy as jnp
from jax import lax
from jax.experimental import pallas as pl
from jax.experimental.pallas import tpu as pltpu
from jax.sharding import Mesh
from jax.sharding import PartitionSpec as P

ROW = ("row_0", "row_1")
COL = ("col_0", "col_1")
Z = "col_0"
CORE = "col_1"
F32 = jnp.float32
BF16 = jnp.bfloat16
LANES = 128
SUBLANES = 8
MIB = 1 << 20
VMEM = pl.BlockSpec(memory_space=pltpu.VMEM)
SMEM = pl.BlockSpec(memory_space=pltpu.SMEM)


def dot(left, right, over):
    return lax.dot_general(
        left, right, (((over[0],), (over[1],)), ((), ())), preferred_element_type=F32
    )


def exchange(x, axis):
    return lax.all_to_all(x, axis, 0, 0, tiled=True)


def swap_cores(x):
    return lax.ppermute(x, CORE, [(0, 1), (1, 0)])


def local_kernel(body, out_shape, operands, limit=16, flops=1_000_000):
    return pl.pallas_call(
        body,
        in_specs=[SMEM if a.dtype == jnp.int32 else VMEM for a in operands],
        out_specs=[VMEM] * len(out_shape),
        out_shape=[jax.ShapeDtypeStruct(*shape) for shape in out_shape],
        compiler_params=pltpu.CompilerParams(vmem_limit_bytes=limit * MIB),
        cost_estimate=pl.CostEstimate(flops=flops, bytes_accessed=1_000_000, transcendentals=0),
    )(*operands)


def copies_in_kernel(tokens_ref, dy_ref, out_ref, done):
    rows = tokens_ref.shape[0]
    copies = [
        pltpu.make_async_copy(
            own_ref, out_ref.at[0, kind * rows : (kind + 1) * rows], done.at[kind]
        )
        for kind, own_ref in enumerate((tokens_ref, dy_ref))
    ]
    for copy in copies:
        copy.start()
    for copy in copies:
        copy.wait()
    both = out_ref[0]
    for peer in range(1, out_ref.shape[0]):
        out_ref[peer] = both


def copies_in(tokens, grad_out, sources):
    rows, depth = tokens.shape
    return pl.pallas_call(
        copies_in_kernel,
        in_specs=[pl.BlockSpec(memory_space=pl.ANY)] * 2,
        out_specs=VMEM,
        out_shape=jax.ShapeDtypeStruct((sources, 2 * rows, depth), BF16),
        scratch_shapes=[pltpu.SemaphoreType.DMA((2,))],
        compiler_params=pltpu.CompilerParams(vmem_limit_bytes=4 * MIB),
        cost_estimate=pl.CostEstimate(flops=20_000_000_000, bytes_accessed=1_000_000, transcendentals=0),
        name="copies_in",
    )(tokens, grad_out)


def terms_kernel(
    place_ref, in_ref, wg_ref, wu_ref, wd_ref, theirs_ref, mine_ref, ord_ref, prod_ref
):
    steps = wg_ref.shape[1] // LANES
    peers = theirs_ref.shape[0]
    sources, rows2, depth = in_ref.shape
    rows = rows2 // 2
    tokens = sources * rows
    half = tokens // 2
    part = LANES // peers
    width = steps * part
    core = place_ref[0]
    sides = ((1 - core, theirs_ref), (core, mine_ref))
    x = in_ref[:, :rows, :].reshape(tokens, depth)

    def multiply(step):
        lanes = slice(step * LANES, (step + 1) * LANES)
        w = jnp.concatenate([wg_ref[:, lanes], wu_ref[:, lanes]], 1)
        prod_ref[step % 2] = jnp.dot(x, w, preferred_element_type=F32)

    def turn(step):
        at = step * part
        for side, out_ref in sides:
            token_at = pl.multiple_of(side * half, half)
            block = prod_ref[step % 2, pl.ds(token_at, half), :].T.astype(BF16)
            out_ref[:, at : at + part, :] = block[:LANES].reshape(peers, part, half)
            out_ref[:, width + at : width + at + part, :] = block[LANES:].reshape(peers, part, half)

    for step in range(steps):
        multiply(step)
        if step:
            turn(step - 1)
    for at, side in ((0, 1 - core), (half, core)):
        own = in_ref[pl.ds(side * (sources // 2), sources // 2), rows:, :]
        ord_ref[at : at + half] = own.reshape(half, depth)
    turn(steps - 1)
    for first in range(0, steps, 4):
        end = min(first + 4, steps)
        block = dot(wd_ref[first * LANES : end * LANES], ord_ref[...], (1, 1)).astype(BF16)
        for step in range(first, end):
            piece = block[(step - first) * LANES : (step - first + 1) * LANES]
            piece = piece.reshape(peers, part, tokens)
            to = 2 * width + step * part
            theirs_ref[:, to : to + part, :] = piece[:, :, :half]
            mine_ref[:, to : to + part, :] = piece[:, :, half:]


def terms(place, fetched, w_gate, w_up, w_down, peers):
    depth, hidden = w_gate.shape
    tokens = fetched.shape[0] * fetched.shape[1] // 2
    out = jax.ShapeDtypeStruct((peers, 3 * hidden // peers, tokens // 2), BF16)
    dy = jax.ShapeDtypeStruct((tokens, depth), BF16)
    return pl.pallas_call(
        terms_kernel,
        in_specs=[SMEM] + [VMEM] * 4,
        out_specs=[VMEM] * 3,
        out_shape=[out, out, dy],
        scratch_shapes=[pltpu.VMEM((2, tokens, 2 * LANES), F32)],
        compiler_params=pltpu.CompilerParams(vmem_limit_bytes=TERMS_MIB * MIB),
        cost_estimate=pl.CostEstimate(
            flops=6 * tokens * depth * hidden, bytes_accessed=6 * depth * hidden, transcendentals=0
        ),
        name="terms",
    )(place, fetched, w_gate, w_up, w_down)


def gram_kernel(place_ref, in_ref, theirs_ref, mine_ref):
    sources, rows2, depth = in_ref.shape
    rows = rows2 // 2
    half = sources * rows // 2
    core, row = place_ref[0], place_ref[2]
    for side, out_ref in ((1 - core, theirs_ref), (core, mine_ref)):
        for kind in range(2):
            at = slice(kind * rows, (kind + 1) * rows)
            every = in_ref[pl.ds(side * (sources // 2), sources // 2), at, :]
            out_ref[at] = dot(in_ref[row, at], every.reshape(half, depth), (1, 1)).astype(BF16)


def gram_sum_kernel(*refs):
    *terms_in, out_ref = refs
    total = terms_in[0][...].astype(F32)
    for ref in terms_in[1:]:
        total = total + ref[...].astype(F32)
    total = total.astype(BF16)
    if len(out_ref.shape) == 2:
        out_ref[...] = total
    else:
        for peer in range(out_ref.shape[0]):
            out_ref[peer] = total


def gram_table_kernel(parts_ref, table_ref):
    sources, rows2, half = parts_ref.shape
    rows = rows2 // 2
    for kind in range(2):
        part = parts_ref[:, kind * rows : (kind + 1) * rows, :]
        table_ref[kind] = part.reshape(sources * rows, half)


def split_kernel(place_ref, mine_ref, arrived_ref, first_ref, second_ref, keep_ref):
    parity = lax.rem(place_ref[1], 2)
    cut = first_ref.shape[1]
    for q in range(keep_ref.shape[0]):
        away, here = 2 * q + 1 - parity, 2 * q + parity
        sent = (mine_ref[away].astype(F32) + arrived_ref[away].astype(F32)).astype(BF16)
        first_ref[q] = sent[:cut]
        second_ref[q] = sent[cut:]
        keep_ref[q] = mine_ref[here].astype(F32) + arrived_ref[here].astype(F32)


def pair_kernel(place_ref, keep_ref, first_ref, second_ref, own_ref, up_ref, down_ref, far_ref):
    count = keep_ref.shape[0]
    cut = first_ref.shape[1]
    q0 = place_ref[1] // 2
    for shift, out_ref in ((0, own_ref), (1, up_ref), (count - 1, down_ref), (2, far_ref)):
        q = lax.rem(q0 + shift, count)
        out_ref[:cut] = (keep_ref[q, :cut] + first_ref[q].astype(F32)).astype(out_ref.dtype)
        out_ref[cut:] = (keep_ref[q, cut:] + second_ref[q].astype(F32)).astype(out_ref.dtype)


def acts_kernel(own_ref, up_in, down_in, far_in, gate_ref, up_ref, acts_ref):
    width = gate_ref.shape[0]
    total = own_ref[...] + up_in[...].astype(F32)
    total = total + down_in[...].astype(F32) + far_in[...].astype(F32)
    gate, up = total[:width], total[width : 2 * width]
    grad_hidden = total[2 * width :].astype(BF16).astype(F32)
    sig = jax.nn.sigmoid(gate)
    silu = gate * sig
    gate_ref[...] = gate
    up_ref[...] = up
    acts_ref[:width] = (grad_hidden * up * sig * (1.0 + gate * (1.0 - sig))).astype(BF16)
    acts_ref[width : 2 * width] = (grad_hidden * silu).astype(BF16)
    acts_ref[2 * width :] = (silu * up).astype(BF16)


def step_kernel(place_ref, acts_ref, arrived_ref, grams_ref, step_ref, local_ref):
    half = grams_ref.shape[2]
    width = acts_ref.shape[0] // 3
    core = place_ref[0]
    kinds = ((0, 2 * width, 0), (2 * width, 3 * width, 1))
    local = 0.0
    for first, end, kind in kinds:
        product = 0.0
        for side, part_ref in ((1 - core, arrived_ref), (core, acts_ref)):
            gram = grams_ref[kind, pl.ds(pl.multiple_of(side * half, half), half), :]
            product += dot(part_ref[first:end], gram, (1, 0))
        local += jnp.sum(acts_ref[first:end].astype(F32) * product)
        if first == 0:
            step_ref[...] = product
    local_ref[...] = jnp.full(local_ref.shape, local, F32)


def norm_kernel(plane_ref, acts_ref, out_ref):
    peers, _, _ = out_ref.shape
    width = acts_ref.shape[0] // 3
    plane = plane_ref[0]
    for peer in range(1, plane_ref.shape[0]):
        plane = plane + plane_ref[peer]
    high = plane.astype(BF16).astype(F32)
    pair = jnp.concatenate([high, plane - high], 0).astype(BF16)
    hidden = acts_ref[2 * width :]
    for peer in range(peers):
        out_ref[peer, :width] = hidden
        out_ref[peer, width:] = pair


def pert_kernel(ends_ref, gate_ref, up_ref, step_ref, radius_ref, out_ref, scale_ref, norm_ref):
    peers, _, lanes = ends_ref.shape
    width = gate_ref.shape[0]
    total = jnp.zeros((SUBLANES, lanes), F32)
    for peer in range(peers):
        pair = ends_ref[peer, width:].astype(F32)
        total = total + (pair[:SUBLANES] + pair[SUBLANES:])
    scale = radius_ref[...] * lax.rsqrt(total + 1e-06)
    norm_ref[...] = jnp.sqrt(total)[:1, :1]
    scale_ref[...] = scale
    pgate = gate_ref[...] + scale[:1] * step_ref[:width]
    pup = up_ref[...] + scale[:1] * step_ref[width:]
    phidden = (pgate * jax.nn.sigmoid(pgate) * pup).astype(BF16)
    for peer in range(peers):
        out_ref[peer] = phidden


def out_kernel(
    place_ref, scale_ref, pt_ref, pm_ref, ht_ref, hm_ref, wd_ref, dy_ref, out_ref, ph_ref, mix_ref
):
    peers, width, half = pm_ref.shape
    part = LANES // peers
    for a, p_ref in ((0, pt_ref), (half, pm_ref)):
        for b, h_ref in ((0, ht_ref), (half, hm_ref)):
            p = p_ref[...].reshape(peers * width, half)
            h = h_ref[:, :width, :].reshape(peers * width, half)
            mix = scale_ref[:1] * dot(p, h, (0, 0))
            mix_ref[a : a + half, b : b + half] = mix.astype(BF16)
    for at, p_ref in ((0, pt_ref), (half, pm_ref)):
        for j in range(width // part):
            block = p_ref[:, j * part : (j + 1) * part, :].reshape(LANES, half)
            ph_ref[at : at + half, j * LANES : (j + 1) * LANES] = block.astype(F32).T.astype(BF16)
    theirs = pl.multiple_of((1 - place_ref[0]) * half, half)
    mine = pl.multiple_of(place_ref[0] * half, half)
    depth = dy_ref.shape[1]
    block = min(depth, 256)
    for first in range(0, depth, block):
        lanes = slice(first, first + block)
        acc = dot(ph_ref[...], wd_ref[:, lanes], (1, 0)) + dot(mix_ref[...], dy_ref[:, lanes], (1, 0))
        out = acc.astype(BF16)
        out_ref[pl.ds(theirs, half), lanes] = out[:half]
        out_ref[pl.ds(mine, half), lanes] = out[half:]


def out_terms(place, scale, ph_theirs, ph_mine, h_theirs, h_mine, w_down, dy):
    hidden, depth = w_down.shape
    tokens = dy.shape[0]
    return pl.pallas_call(
        out_kernel,
        in_specs=[SMEM] + [VMEM] * 7,
        out_specs=VMEM,
        out_shape=jax.ShapeDtypeStruct((tokens, depth), BF16),
        scratch_shapes=[pltpu.VMEM((tokens, hidden), BF16), pltpu.VMEM((tokens, tokens), BF16)],
        compiler_params=pltpu.CompilerParams(vmem_limit_bytes=24 * MIB),
        cost_estimate=pl.CostEstimate(
            flops=2 * tokens * depth * hidden, bytes_accessed=2 * depth * hidden, transcendentals=0
        ),
        name="out_terms",
    )(place, scale, ph_theirs, ph_mine, h_theirs, h_mine, w_down, dy)


def per_device(tokens, grad_out, w_gate, w_up, w_down, radius):
    peers = lax.axis_size(Z)
    sources = lax.axis_size(ROW)
    rows, depth = tokens.shape
    half = sources * rows // 2
    width = w_gate.shape[1] // peers
    every = 3 * width
    cut = (every + 31) // 32 * 16
    neighbour = [(z, z ^ 1) for z in range(peers)]
    other = [(z, (z + 2 * (z % 2) - 1) % peers) for z in range(peers)]

    def moved(x, by):
        return lax.ppermute(x, Z, [(z, (z + by) % peers) for z in range(peers)])

    radius = jnp.broadcast_to(radius, (SUBLANES, half))
    place = jnp.stack([lax.axis_index(axis) for axis in (CORE, Z, ROW)]).astype(jnp.int32)
    tokens, grad_out, place, radius = lax.optimization_barrier((tokens, grad_out, place, radius))
    fetched = exchange(copies_in(tokens, grad_out, sources), ROW)
    flat = ((2 * rows, half), BF16)
    theirs, gram = local_kernel(gram_kernel, [flat, flat], (place, fetched))
    fetched, theirs = lax.optimization_barrier((fetched, theirs))
    theirs = swap_cores(theirs)
    theirs_wide, mine, dy = terms(place, fetched, w_gate, w_up, w_down, peers)
    (gram,) = local_kernel(gram_sum_kernel, [flat], (gram, theirs))
    theirs_wide, gram = lax.optimization_barrier((theirs_wide, gram))
    arrived = swap_cores(theirs_wide)
    theirs = lax.ppermute(gram, Z, neighbour)
    (gram,) = local_kernel(gram_sum_kernel, [flat], (gram, theirs))
    first, second, keep = local_kernel(
        split_kernel,
        [
            ((peers // 2, cut, half), BF16),
            ((peers // 2, every - cut, half), BF16),
            ((peers // 2, every, half), F32),
        ],
        (place, mine, arrived),
    )
    first = lax.ppermute(first, Z, neighbour)
    second = lax.ppermute(second, Z, other)
    others = (moved(gram, 2), moved(gram, -2), moved(gram, 4))
    (grams,) = local_kernel(gram_sum_kernel, [((sources, 2 * rows, half), BF16)], (gram, *others))
    block = ((every, half), BF16)
    own, up_block, down_block, far_block = local_kernel(
        pair_kernel, [((every, half), F32), block, block, block], (place, keep, first, second)
    )
    blocks = (moved(up_block, 2), moved(down_block, -2), moved(far_block, 4))
    grams = exchange(grams, ROW)
    (sums,) = local_kernel(gram_table_kernel, [((2, 2 * half, half), BF16)], (grams,))
    gate, up, acts = local_kernel(
        acts_kernel,
        [
            ((width, half), F32),
            ((width, half), F32),
            ((3 * width, half), BF16),
        ],
        (own, *blocks),
    )
    arrived = swap_cores(acts)
    step, local = local_kernel(
        step_kernel,
        [((2 * width, half), F32), ((2 * sources, SUBLANES, LANES), F32)],
        (place, acts, arrived, sums),
    )
    plane = exchange(local, (*ROW, CORE))
    (sent,) = local_kernel(
        norm_kernel, [((peers, width + 2 * SUBLANES, half), BF16)], (plane, acts)
    )
    h_mine = exchange(sent, Z)
    tile = ((SUBLANES, half), F32)
    sent, scale, norm = local_kernel(
        pert_kernel,
        [((peers, width, half), BF16), tile, ((1, 1), F32)],
        (h_mine, gate, up, step, radius),
    )
    ph_mine = exchange(sent, Z)
    ph_mine, h_mine = lax.optimization_barrier((ph_mine, h_mine))
    ph_theirs = swap_cores(ph_mine)
    h_theirs = swap_cores(h_mine)
    partial_out = out_terms(place, scale, ph_theirs, ph_mine, h_theirs, h_mine, w_down, dy)
    partial_out, norm = lax.optimization_barrier((partial_out, norm.reshape(1)))
    parts = exchange(partial_out.reshape(sources, rows, depth), ROW)
    return (jnp.sum(parts.astype(F32), 0).astype(BF16), norm)


TERMS_MIB = 24


def solution(mesh):
    split = Mesh(mesh.devices.reshape(4, 4, 8, 2), ("row_0", "row_1", "col_0", "col_1"))
    return jax.shard_map(
        per_device,
        mesh=split,
        in_specs=(P(ROW, COL), P(ROW, COL), P(COL, ROW), P(COL, ROW), P(ROW, COL), P()),
        out_specs=(P(ROW, COL), P()),
        check_vma=False,
    )
```

```python
import jax
import jax.numpy as jnp
from jax import lax
from jax.experimental import pallas as pl
from jax.experimental.pallas import tpu as pltpu
from jax.sharding import Mesh
from jax.sharding import PartitionSpec as P

ROW = ("row_0", "row_1")
COL = ("col_0", "col_1")
Z = "col_0"
CORE = "col_1"
F32 = jnp.float32
BF16 = jnp.bfloat16
LANES = 128
SUBLANES = 8
MIB = 1 << 20
VMEM = pl.BlockSpec(memory_space=pltpu.VMEM)
SMEM = pl.BlockSpec(memory_space=pltpu.SMEM)


def dot(left, right, over):
    return lax.dot_general(
        left, right, (((over[0],), (over[1],)), ((), ())), preferred_element_type=F32
    )


def exchange(x, axis):
    return lax.all_to_all(x, axis, 0, 0, tiled=True)


def swap_cores(x):
    return lax.ppermute(x, CORE, [(0, 1), (1, 0)])


def local_kernel(body, out_shape, operands, limit=16, flops=1_000_000):
    return pl.pallas_call(
        body,
        in_specs=[SMEM if a.dtype == jnp.int32 else VMEM for a in operands],
        out_specs=[VMEM] * len(out_shape),
        out_shape=[jax.ShapeDtypeStruct(*shape) for shape in out_shape],
        compiler_params=pltpu.CompilerParams(vmem_limit_bytes=limit * MIB),
        cost_estimate=pl.CostEstimate(flops=flops, bytes_accessed=1_000_000, transcendentals=0),
    )(*operands)


def copies_in_kernel(both_ref, out_ref):
    both = both_ref[...]
    for peer in range(out_ref.shape[0]):
        out_ref[peer] = both


def copies_in(both, sources):
    return pl.pallas_call(
        copies_in_kernel,
        in_specs=[VMEM],
        out_specs=VMEM,
        out_shape=jax.ShapeDtypeStruct((sources, *both.shape), BF16),
        compiler_params=pltpu.CompilerParams(vmem_limit_bytes=4 * MIB),
        cost_estimate=pl.CostEstimate(
            flops=20_000_000_000, bytes_accessed=1_000_000, transcendentals=0
        ),
        name="copies_in",
    )(both)


def terms_kernel(
    place_ref, in_ref, wg_ref, wu_ref, wd_ref, theirs_ref, mine_ref, ord_ref, prod_ref
):
    steps = wg_ref.shape[1] // LANES
    peers = theirs_ref.shape[0]
    sources, rows2, depth = in_ref.shape
    rows = rows2 // 2
    tokens = sources * rows
    half = tokens // 2
    part = LANES // peers
    width = steps * part
    core = place_ref[0]
    sides = ((1 - core, theirs_ref), (core, mine_ref))
    x = in_ref[:, :rows, :].reshape(tokens, depth)

    def multiply(step):
        lanes = slice(step * LANES, (step + 1) * LANES)
        w = jnp.concatenate([wg_ref[:, lanes], wu_ref[:, lanes]], 1)
        prod_ref[step % 2] = jnp.dot(x, w, preferred_element_type=F32)

    def turn(step):
        at = step * part
        for side, out_ref in sides:
            token_at = pl.multiple_of(side * half, half)
            block = prod_ref[step % 2, pl.ds(token_at, half), :].T.astype(BF16)
            out_ref[:, at : at + part, :] = block[:LANES].reshape(peers, part, half)
            out_ref[:, width + at : width + at + part, :] = block[LANES:].reshape(peers, part, half)

    for step in range(steps):
        multiply(step)
        if step:
            turn(step - 1)
    for at, side in ((0, 1 - core), (half, core)):
        own = in_ref[pl.ds(side * (sources // 2), sources // 2), rows:, :]
        ord_ref[at : at + half] = own.reshape(half, depth)
    turn(steps - 1)
    for first in range(0, steps, 4):
        end = min(first + 4, steps)
        block = dot(wd_ref[first * LANES : end * LANES], ord_ref[...], (1, 1)).astype(BF16)
        for step in range(first, end):
            piece = block[(step - first) * LANES : (step - first + 1) * LANES]
            piece = piece.reshape(peers, part, tokens)
            to = 2 * width + step * part
            theirs_ref[:, to : to + part, :] = piece[:, :, :half]
            mine_ref[:, to : to + part, :] = piece[:, :, half:]


def terms(place, fetched, w_gate, w_up, w_down, peers):
    depth, hidden = w_gate.shape
    tokens = fetched.shape[0] * fetched.shape[1] // 2
    out = jax.ShapeDtypeStruct((peers, 3 * hidden // peers, tokens // 2), BF16)
    dy = jax.ShapeDtypeStruct((tokens, depth), BF16)
    return pl.pallas_call(
        terms_kernel,
        in_specs=[SMEM] + [VMEM] * 4,
        out_specs=[VMEM] * 3,
        out_shape=[out, out, dy],
        scratch_shapes=[pltpu.VMEM((2, tokens, 2 * LANES), F32)],
        compiler_params=pltpu.CompilerParams(vmem_limit_bytes=TERMS_MIB * MIB),
        cost_estimate=pl.CostEstimate(
            flops=6 * tokens * depth * hidden, bytes_accessed=6 * depth * hidden, transcendentals=0
        ),
        name="terms",
    )(place, fetched, w_gate, w_up, w_down)


def gram_kernel(place_ref, in_ref, theirs_ref, mine_ref):
    sources, rows2, depth = in_ref.shape
    rows = rows2 // 2
    half = sources * rows // 2
    core, row = place_ref[0], place_ref[2]
    for side, out_ref in ((1 - core, theirs_ref), (core, mine_ref)):
        for kind in range(2):
            at = slice(kind * rows, (kind + 1) * rows)
            every = in_ref[pl.ds(side * (sources // 2), sources // 2), at, :]
            out_ref[at] = dot(in_ref[row, at], every.reshape(half, depth), (1, 1)).astype(BF16)


def gram_sum_kernel(*refs):
    *terms_in, out_ref = refs
    total = terms_in[0][...].astype(F32)
    for ref in terms_in[1:]:
        total = total + ref[...].astype(F32)
    total = total.astype(BF16)
    if len(out_ref.shape) == 2:
        out_ref[...] = total
    else:
        for peer in range(out_ref.shape[0]):
            out_ref[peer] = total


def gram_table_kernel(parts_ref, table_ref):
    sources, rows2, half = parts_ref.shape
    rows = rows2 // 2
    for kind in range(2):
        part = parts_ref[:, kind * rows : (kind + 1) * rows, :]
        table_ref[kind] = part.reshape(sources * rows, half)


def split_kernel(place_ref, mine_ref, arrived_ref, first_ref, second_ref, keep_ref):
    parity = lax.rem(place_ref[1], 2)
    cut = first_ref.shape[1]
    for q in range(keep_ref.shape[0]):
        away, here = 2 * q + 1 - parity, 2 * q + parity
        sent = (mine_ref[away].astype(F32) + arrived_ref[away].astype(F32)).astype(BF16)
        first_ref[q] = sent[:cut]
        second_ref[q] = sent[cut:]
        keep_ref[q] = mine_ref[here].astype(F32) + arrived_ref[here].astype(F32)


def pair_kernel(place_ref, keep_ref, first_ref, second_ref, own_ref, up_ref, down_ref, far_ref):
    count = keep_ref.shape[0]
    cut = first_ref.shape[1]
    q0 = place_ref[1] // 2
    for shift, out_ref in ((0, own_ref), (1, up_ref), (count - 1, down_ref), (2, far_ref)):
        q = lax.rem(q0 + shift, count)
        out_ref[:cut] = (keep_ref[q, :cut] + first_ref[q].astype(F32)).astype(out_ref.dtype)
        out_ref[cut:] = (keep_ref[q, cut:] + second_ref[q].astype(F32)).astype(out_ref.dtype)


def acts_kernel(own_ref, up_in, down_in, far_in, gate_ref, up_ref, acts_ref):
    width = gate_ref.shape[0]
    total = own_ref[...] + up_in[...].astype(F32)
    total = total + down_in[...].astype(F32) + far_in[...].astype(F32)
    gate, up = total[:width], total[width : 2 * width]
    grad_hidden = total[2 * width :].astype(BF16).astype(F32)
    sig = jax.nn.sigmoid(gate)
    silu = gate * sig
    gate_ref[...] = gate
    up_ref[...] = up
    acts_ref[:width] = (grad_hidden * up * sig * (1.0 + gate * (1.0 - sig))).astype(BF16)
    acts_ref[width : 2 * width] = (grad_hidden * silu).astype(BF16)
    acts_ref[2 * width :] = (silu * up).astype(BF16)


def step_kernel(place_ref, acts_ref, arrived_ref, grams_ref, step_ref, local_ref):
    half = grams_ref.shape[2]
    width = acts_ref.shape[0] // 3
    core = place_ref[0]
    kinds = ((0, 2 * width, 0), (2 * width, 3 * width, 1))
    local = 0.0
    for first, end, kind in kinds:
        product = 0.0
        for side, part_ref in ((1 - core, arrived_ref), (core, acts_ref)):
            gram = grams_ref[kind, pl.ds(pl.multiple_of(side * half, half), half), :]
            product += dot(part_ref[first:end], gram, (1, 0))
        local += jnp.sum(acts_ref[first:end].astype(F32) * product)
        if first == 0:
            step_ref[...] = product
    local_ref[...] = jnp.full(local_ref.shape, local, F32)


def norm_kernel(plane_ref, acts_ref, out_ref):
    peers, _, _ = out_ref.shape
    width = acts_ref.shape[0] // 3
    plane = plane_ref[0]
    for peer in range(1, plane_ref.shape[0]):
        plane = plane + plane_ref[peer]
    high = plane.astype(BF16).astype(F32)
    pair = jnp.concatenate([high, plane - high], 0).astype(BF16)
    hidden = acts_ref[2 * width :]
    for peer in range(peers):
        out_ref[peer, :width] = hidden
        out_ref[peer, width:] = pair


def pert_kernel(ends_ref, gate_ref, up_ref, step_ref, radius_ref, out_ref, scale_ref, norm_ref):
    peers, _, lanes = ends_ref.shape
    width = gate_ref.shape[0]
    total = jnp.zeros((SUBLANES, lanes), F32)
    for peer in range(peers):
        pair = ends_ref[peer, width:].astype(F32)
        total = total + (pair[:SUBLANES] + pair[SUBLANES:])
    scale = radius_ref[...] * lax.rsqrt(total + 1e-06)
    norm_ref[...] = jnp.sqrt(total)[:1, :1]
    scale_ref[...] = scale
    pgate = gate_ref[...] + scale[:1] * step_ref[:width]
    pup = up_ref[...] + scale[:1] * step_ref[width:]
    phidden = (pgate * jax.nn.sigmoid(pgate) * pup).astype(BF16)
    for peer in range(peers):
        out_ref[peer] = phidden


def out_kernel(
    place_ref, scale_ref, pt_ref, pm_ref, ht_ref, hm_ref, wd_ref, dy_ref, out_ref, ph_ref, mix_ref
):
    peers, width, half = pm_ref.shape
    part = LANES // peers
    for a, p_ref in ((0, pt_ref), (half, pm_ref)):
        for b, h_ref in ((0, ht_ref), (half, hm_ref)):
            p = p_ref[...].reshape(peers * width, half)
            h = h_ref[:, :width, :].reshape(peers * width, half)
            mix = scale_ref[:1] * dot(p, h, (0, 0))
            mix_ref[a : a + half, b : b + half] = mix.astype(BF16)
    for at, p_ref in ((0, pt_ref), (half, pm_ref)):
        for j in range(width // part):
            block = p_ref[:, j * part : (j + 1) * part, :].reshape(LANES, half)
            ph_ref[at : at + half, j * LANES : (j + 1) * LANES] = block.astype(F32).T.astype(BF16)
    theirs = pl.multiple_of((1 - place_ref[0]) * half, half)
    mine = pl.multiple_of(place_ref[0] * half, half)
    depth = dy_ref.shape[1]
    block = min(depth, 256)
    for first in range(0, depth, block):
        lanes = slice(first, first + block)
        acc = dot(ph_ref[...], wd_ref[:, lanes], (1, 0)) + dot(mix_ref[...], dy_ref[:, lanes], (1, 0))
        out = acc.astype(BF16)
        out_ref[pl.ds(theirs, half), lanes] = out[:half]
        out_ref[pl.ds(mine, half), lanes] = out[half:]


def out_terms(place, scale, ph_theirs, ph_mine, h_theirs, h_mine, w_down, dy):
    hidden, depth = w_down.shape
    tokens = dy.shape[0]
    return pl.pallas_call(
        out_kernel,
        in_specs=[SMEM] + [VMEM] * 7,
        out_specs=VMEM,
        out_shape=jax.ShapeDtypeStruct((tokens, depth), BF16),
        scratch_shapes=[pltpu.VMEM((tokens, hidden), BF16), pltpu.VMEM((tokens, tokens), BF16)],
        compiler_params=pltpu.CompilerParams(vmem_limit_bytes=24 * MIB),
        cost_estimate=pl.CostEstimate(
            flops=2 * tokens * depth * hidden, bytes_accessed=2 * depth * hidden, transcendentals=0
        ),
        name="out_terms",
    )(place, scale, ph_theirs, ph_mine, h_theirs, h_mine, w_down, dy)


def per_device(tokens, grad_out, w_gate, w_up, w_down, radius):
    peers = lax.axis_size(Z)
    sources = lax.axis_size(ROW)
    rows, depth = tokens.shape
    half = sources * rows // 2
    width = w_gate.shape[1] // peers
    every = 3 * width
    cut = (every + 31) // 32 * 16
    neighbour = [(z, z ^ 1) for z in range(peers)]
    other = [(z, (z + 2 * (z % 2) - 1) % peers) for z in range(peers)]

    def moved(x, by):
        return lax.ppermute(x, Z, [(z, (z + by) % peers) for z in range(peers)])

    radius = jnp.broadcast_to(radius, (SUBLANES, half))
    place = jnp.stack([lax.axis_index(axis) for axis in (CORE, Z, ROW)]).astype(jnp.int32)
    both = jnp.concatenate([tokens, grad_out], 0)
    both, place, radius = lax.optimization_barrier((both, place, radius))
    fetched = exchange(copies_in(both, sources), ROW)
    flat = ((2 * rows, half), BF16)
    theirs, gram = local_kernel(gram_kernel, [flat, flat], (place, fetched))
    fetched, theirs = lax.optimization_barrier((fetched, theirs))
    theirs = swap_cores(theirs)
    theirs_wide, mine, dy = terms(place, fetched, w_gate, w_up, w_down, peers)
    (gram,) = local_kernel(gram_sum_kernel, [flat], (gram, theirs))
    theirs_wide, gram = lax.optimization_barrier((theirs_wide, gram))
    arrived = swap_cores(theirs_wide)
    theirs = lax.ppermute(gram, Z, neighbour)
    (gram,) = local_kernel(gram_sum_kernel, [flat], (gram, theirs))
    first, second, keep = local_kernel(
        split_kernel,
        [
            ((peers // 2, cut, half), BF16),
            ((peers // 2, every - cut, half), BF16),
            ((peers // 2, every, half), F32),
        ],
        (place, mine, arrived),
    )
    first = lax.ppermute(first, Z, neighbour)
    second = lax.ppermute(second, Z, other)
    others = (moved(gram, 2), moved(gram, -2), moved(gram, 4))
    (grams,) = local_kernel(gram_sum_kernel, [((sources, 2 * rows, half), BF16)], (gram, *others))
    block = ((every, half), BF16)
    own, up_block, down_block, far_block = local_kernel(
        pair_kernel, [((every, half), F32), block, block, block], (place, keep, first, second)
    )
    blocks = (moved(up_block, 2), moved(down_block, -2), moved(far_block, 4))
    grams = exchange(grams, ROW)
    (sums,) = local_kernel(gram_table_kernel, [((2, 2 * half, half), BF16)], (grams,))
    gate, up, acts = local_kernel(
        acts_kernel,
        [
            ((width, half), F32),
            ((width, half), F32),
            ((3 * width, half), BF16),
        ],
        (own, *blocks),
    )
    arrived = swap_cores(acts)
    step, local = local_kernel(
        step_kernel,
        [((2 * width, half), F32), ((2 * sources, SUBLANES, LANES), F32)],
        (place, acts, arrived, sums),
    )
    plane = exchange(local, (*ROW, CORE))
    (sent,) = local_kernel(
        norm_kernel, [((peers, width + 2 * SUBLANES, half), BF16)], (plane, acts)
    )
    h_mine = exchange(sent, Z)
    tile = ((SUBLANES, half), F32)
    sent, scale, norm = local_kernel(
        pert_kernel,
        [((peers, width, half), BF16), tile, ((1, 1), F32)],
        (h_mine, gate, up, step, radius),
    )
    ph_mine = exchange(sent, Z)
    ph_theirs = swap_cores(ph_mine)
    h_theirs = swap_cores(h_mine)
    partial_out = out_terms(place, scale, ph_theirs, ph_mine, h_theirs, h_mine, w_down, dy)
    partial_out, norm = lax.optimization_barrier((partial_out, norm.reshape(1)))
    parts = exchange(partial_out.reshape(sources, rows, depth), ROW)
    return (jnp.sum(parts.astype(F32), 0).astype(BF16), norm)


TERMS_MIB = 24


def solution(mesh):
    split = Mesh(mesh.devices.reshape(4, 4, 8, 2), ("row_0", "row_1", "col_0", "col_1"))
    return jax.shard_map(
        per_device,
        mesh=split,
        in_specs=(P(ROW, COL), P(ROW, COL), P(COL, ROW), P(COL, ROW), P(ROW, COL), P()),
        out_specs=(P(ROW, COL), P()),
        check_vma=False,
    )
```
